256 devices in a mesh: group: 2 (over y), seq: 64 (over x, z), tensor: 2 (over core).
Axes of the slice: x: 4, y: 2, z: 16, core: 2. Of those that a mesh axis runs over, the one named last changes fastest.
The devices are a block of a 4x16x16 slice.
Arguments:
- query: bfloat16 [32, 64, 128], P('group', 'tensor'), parts along dimension 0, may hold values from -400 to 400
- key_cache: bfloat16 [4096, 128, 8, 128], P(('group', 'seq'), None, 'tensor'), parts along dimension 0, may hold values from -6 to 6
- value_cache: bfloat16 [4096, 128, 8, 128], P(('group', 'seq'), None, 'tensor'), parts along dimension 0, may hold values from -6 to 6
- lengths: int32 [32], P('group'), parts along dimension 0, may hold values from 1 to 32768, 129024 in all
- page_order: int32 [4096], P('group'), parts along dimension 0, may hold values from 0 to 2047, as said below
- out_weight: bfloat16 [8192, 8192], P('tensor', 'seq'), may hold values from -0.59765625 to 0.59765625
Outputs:
- mixed: bfloat16 [32, 8192], P(('group', 'tensor'), 'seq'), parts along dimension 0
The draws below stay inside these ranges and needn't reach their ends.
There are 2 independent parts, one for each index of `group`. The reference program is written for one: setup_inputs(seed, part) draws one part's arguments, and reference() takes and returns one part's arrays. A program takes and returns all parts, laid end to end along the dimension named above; an argument that names none is the same for every part. Nothing has to cross between parts.
Inputs may be any that keep to these rules, and one draw needn't show every extreme that they name: The sequences' lengths sum to 129024; one equals 32768. `page_order`: a permutation of the pages.
All inputs are finite; a program needn't handle non-finite values.
Results may differ from the reference program's by a relative error of at most 0.0065.
Values may be sent and summed in bfloat16 or wider, within the bound.
A program may use at most 64 MiB of HBM per device.

```python
import math
import jax
import jax.numpy as jnp
import numpy as np
from jax import lax

D = 8192
HEADS = 64
KVH = 8
HD = 128
PAGE = 128
PAGES_DEV = 32
SEQS = 16
POOL = 2048
MAXBLK = 256
MAXLEN = 32768
TOTAL = 129024


def draw_key_cache(key, part):
    cached = jax.random.truncated_normal(jax.random.fold_in(key, 21), -6.0, 6.0, (POOL, PAGE, KVH, HD), jnp.float32)
    return cached.astype(jnp.bfloat16)


def draw_query(key, part):
    queries = 1.5 * jax.random.truncated_normal(jax.random.fold_in(key, 31), -4.0, 4.0, (SEQS, HEADS, HD), jnp.float32)
    return queries.astype(jnp.bfloat16)


def draw_page_order(key, part):
    noise = jax.random.randint(jax.random.fold_in(key, 51), (POOL,), 0, 65536)
    page_bias = jax.random.randint(jax.random.fold_in(key, 52), (POOL // PAGES_DEV,), 0, 3)
    device_bias = jnp.repeat(page_bias, PAGES_DEV)
    sort_score = (device_bias * 65536 + noise) * POOL + jnp.arange(POOL, dtype=jnp.int32)
    return jnp.argsort(sort_score, stable=True).astype(jnp.int32)


def block_levels(own_key, shape, split, low, high):
    gain = 1.0
    for axis_at, blocks in split:
        draws = jax.random.uniform(jax.random.fold_in(jax.random.fold_in(own_key, 6), axis_at), (blocks,), jnp.float32, low / len(split), high / len(split))
        gain = gain * jnp.repeat(jnp.exp(draws), shape[axis_at] // blocks).reshape((-1,) + (1,) * (len(shape) - 1 - axis_at))
    return gain


def length_profile(count, total, reach, skew):
    portions = [(1 << 20) // math.isqrt(grade ** skew) + 1 for grade in range(2, count + 1)]
    rest, given = total - reach - (count - 1), [1] * (count - 1)
    while rest > 0:
        free = [i for i in range(count - 1) if given[i] < reach]
        whole, budget = sum([portions[i] for i in free]), rest
        for i in free:
            more = min(reach - given[i], max(1, budget * portions[i] // whole), rest)
            given[i] = given[i] + more
            rest = rest - more
    return np.array([reach] + given)


def ragged(stream_key, amount, total, reach, skew):
    if amount == 2:
        one = jax.random.randint(stream_key, (), max(1, total - reach), min(reach, total - 1) + 1)
        return jnp.stack([one, total - one])
    sizes = jnp.asarray(length_profile(amount, total, reach, skew), jnp.int32)
    pairs = (amount - 1) // 2
    donor, sink = sizes[1:1 + 2 * pairs:2], sizes[2:2 + 2 * pairs:2]
    room = jnp.minimum(donor - 1, reach - sink)
    shifted = jax.random.randint(jax.random.fold_in(stream_key, 1), (pairs,), 0, 1 << 20) % (room + 1)
    sizes = sizes.at[1:1 + 2 * pairs:2].set(donor - shifted).at[2:2 + 2 * pairs:2].set(sink + shifted)
    return sizes[jax.random.permutation(jax.random.fold_in(stream_key, 2), amount)]


def bell_draw(rng, dims, width, bound, cuts=(), kind=jnp.bfloat16):
    result = width * jax.random.normal(rng, dims, jnp.float32)
    if cuts:
        result = result * block_levels(rng, dims, cuts, -0.22, 0.18)
    return jnp.clip(result, -bound, bound).astype(kind)


def setup_inputs(seed: int = 0, part: int = 0) -> dict:
    seeds = jax.random.split(jax.random.key(seed), 7)
    part_splits = jax.random.split(jax.random.fold_in(seeds[6], part), 7)
    query = draw_query(jax.random.fold_in(jax.random.fold_in(seeds[6], part), 71), part)
    key_cache = draw_key_cache(jax.random.fold_in(jax.random.fold_in(seeds[6], part), 71), part)
    value_cache = bell_draw(part_splits[2], (POOL, PAGE, KVH, HD), 1.0, 6.0, ((0, 64), (2, 2)))
    lengths = ragged(part_splits[3], SEQS, TOTAL, MAXLEN, 2).astype(jnp.int32)
    page_order = draw_page_order(jax.random.fold_in(jax.random.fold_in(seeds[6], part), 71), part)
    out_weight = bell_draw(seeds[5], (HEADS * HD, D), 0.1, 0.59765625, ((0, 2), (1, 64)))
    return dict(query=query, key_cache=key_cache, value_cache=value_cache, lengths=lengths, page_order=page_order, out_weight=out_weight)


def reference(query, key_cache, value_cache, lengths, page_order, out_weight):
    counts = (lengths + PAGE - 1) // PAGE
    starts = (jnp.cumsum(counts) - counts).astype(jnp.int32)
    group_size = HEADS // KVH
    score_scale = 1.0 / math.sqrt(HD)

    def per_sequence(inputs):
        seq_query, seq_length, seq_start = inputs
        page_slots = jnp.clip(seq_start + jnp.arange(MAXBLK, dtype=jnp.int32), 0, POOL - 1).astype(jnp.int32)
        page_ids = page_order[page_slots]
        seq_keys = key_cache[page_ids].astype(jnp.float32)
        seq_values = value_cache[page_ids].astype(jnp.float32)
        grouped = seq_query.astype(jnp.float32).reshape(KVH, group_size, HD)
        scores = jnp.einsum('ghd,ptgd->pght', grouped, seq_keys, precision=lax.Precision.HIGHEST) * score_scale
        positions = jnp.arange(MAXBLK, dtype=jnp.int32)[:, None] * PAGE + jnp.arange(PAGE, dtype=jnp.int32)[None, :]
        is_valid = (positions < seq_length)[:, None, None, :]
        scores = jnp.where(is_valid, scores, -1e+30)
        block_max = lax.optimization_barrier(jnp.max(scores, axis=-1))
        weights = jnp.where(is_valid, jnp.exp(scores - block_max[..., None]), 0.0).astype(jnp.bfloat16)
        wide_weights = weights.astype(jnp.float32)
        block_sum = lax.optimization_barrier(jnp.sum(wide_weights, axis=-1))
        block_out = jnp.einsum('pght,ptgd->pghd', wide_weights, seq_values, precision=lax.Precision.HIGHEST)
        largest = lax.optimization_barrier(jnp.max(block_max, axis=0))
        factor = jnp.exp(block_max - largest)
        denominator = lax.optimization_barrier(jnp.sum(factor * block_sum, axis=0))
        numerator = lax.optimization_barrier(jnp.sum(factor[..., None] * block_out, axis=0))
        return (numerator / denominator[..., None]).reshape(HEADS * HD).astype(jnp.bfloat16)
    attended = lax.map(per_sequence, (query, lengths, starts))
    return jnp.dot(attended, out_weight, preferred_element_type=jnp.float32).astype(jnp.bfloat16)
```

```python
import functools
import math

import jax
import jax.numpy as jnp
from jax import lax
from jax.experimental import pallas as pl
from jax.experimental.pallas import tpu as pltpu
from jax.sharding import PartitionSpec as P

MESH = pl.DeviceIdType.MESH
F32 = jnp.float32
BF16 = jnp.bfloat16
I32 = jnp.int32
LANES = 128
NEG = -1e30
PAGES_PER_STEP = 8


def kernel(
    dims,
    len_s, q_hbm, k_hbm, v_hbm, po_hbm, w_hbm, out_ref,
    q_v, k_v, v_v, po_v, w_v, val_v, meta_v, meta_s, cmod_v,
    mrun, lrun, orun, ofin,
    s1o, s1m, r1o, r1m, s2o, s2m, r2o, r2m, g_v, acc_v,
    q_sem, k_sem, v_sem, po_sem, w_sem, meta_sem,
    ws_sem, wr_sem, s1s_sem, s1r_sem, s1ms_sem, s1mr_sem,
    s2s_sem, s2r_sem, s2ms_sem, s2mr_sem, gzs_sem, gzr_sem, gxs_sem, gxr_sem,
):
    nx, nz, pages, page_len, kvh, ns, hl, hd, cores = dims
    rows = page_len * kvh
    hq = hl // nx
    sb = ns // cores
    group_size = hl // kvh
    scale = math.log2(math.e) / math.sqrt(hd)
    me = lax.axis_index("seq")
    t = lax.axis_index("tensor")
    x = me // nz
    z = me % nz
    steps = pages // PAGES_PER_STEP

    xpeers = []
    for dx in range(nx):
        for dt in range(cores):
            if dx or dt:
                xpeers.append(((x + dx) % nx, (t + dt) % cores))
    order = []
    for d in range(nz // 2, 0, -1):
        order.append(d)
        if d != nz - d:
            order.append(nz - d)

    def at(px, pz, pt):
        return {"seq": px * nz + pz, "tensor": pt}

    barrier = pltpu.get_barrier_semaphore()
    for px, pt in xpeers:
        pl.semaphore_signal(barrier, inc=1, device_id=at(px, z, pt), device_id_type=MESH)
    for d in order:
        pl.semaphore_signal(barrier, inc=1, device_id=at(x, (z + d) % nz, t), device_id_type=MESH)

    po_copy = pltpu.make_async_copy(po_hbm, po_v, po_sem)
    po_copy.start()
    q_copy = pltpu.make_async_copy(q_hbm, q_v, q_sem)
    q_copy.start()
    step_rows = PAGES_PER_STEP * rows

    def kv_copy(src, dst, sem, c):
        part = pl.ds(c * step_rows, step_rows)
        return pltpu.make_async_copy(src.at[part], dst.at[part], sem.at[c])

    for c in range(steps):
        kv_copy(k_hbm, k_v, k_sem, c).start()
        kv_copy(v_hbm, v_v, v_sem, c).start()
    w_copy = pltpu.make_async_copy(w_hbm, w_v.at[t], w_sem)
    w_copy.start()

    lens = [len_s[s] for s in range(ns)]
    starts = []
    run = jnp.int32(0)
    for s in range(ns):
        starts.append(run)
        run = run + lax.shift_right_logical(lens[s] + (page_len - 1), int(math.log2(page_len)))
    pr = po_v.shape[0]
    rank = lax.broadcasted_iota(I32, (pr, LANES), 0) * LANES + lax.broadcasted_iota(I32, (pr, LANES), 1)
    owner = jnp.zeros((pr, LANES), I32)
    end = jnp.full((pr, LANES), lens[0], I32)
    for s in range(1, ns):
        past = rank >= starts[s]
        owner = jnp.where(past, s, owner)
        end = jnp.where(past, lens[s] + starts[s] * page_len, end)
    valid = jnp.clip(end - rank * page_len, 0, page_len)
    owner = jnp.where(valid > 0, owner, ns)
    val_v[...] = (owner * 256 + valid).astype(F32)

    cl = lax.broadcasted_iota(I32, (hl, rows), 1)
    hr = lax.broadcasted_iota(I32, (hl, rows), 0)
    cmod_v[...] = jnp.where(cl % kvh == hr // group_size, cl, 1 << 20)
    mrun[0] = jnp.full((hl, LANES), NEG, F32)
    lrun[0] = jnp.zeros((hl, LANES), F32)
    orun[0] = jnp.zeros((hl, hd), F32)

    po_copy.wait()
    ids = lax.broadcasted_iota(I32, (pages, LANES), 0) + me * pages
    acc = jnp.zeros((pages, LANES), F32)
    for i in range(pr):
        hit = jnp.broadcast_to(po_v[i : i + 1, :], (pages, LANES)) == ids
        acc = acc + jnp.where(hit, jnp.broadcast_to(val_v[i : i + 1, :], (pages, LANES)), 0.0)
    val_col = jnp.broadcast_to(jnp.sum(acc, axis=1, keepdims=True), (pages, LANES))
    pad = jnp.concatenate([val_col, jnp.zeros((LANES - pages, LANES), F32)], axis=0)
    val_row = jnp.transpose(pad)[0:1, :]
    own_col = lax.shift_right_logical(val_col.astype(I32), 8)
    val_row_i = val_row.astype(I32)
    own_row = lax.shift_right_logical(val_row_i, 8)
    prow = lax.broadcasted_iota(I32, (pages, LANES), 0)
    lane = lax.broadcasted_iota(I32, (pages, LANES), 1)
    same = (own_col == jnp.broadcast_to(own_row, (pages, LANES))) & (prow < lane)
    prev = jnp.max(jnp.where(same, (prow + 1).astype(F32), 0.0), axis=0, keepdims=True).astype(I32)
    last = jnp.max(jnp.where(own_col == lane, (prow + 1).astype(F32), 0.0), axis=0, keepdims=True).astype(I32)
    meta_v[0:1, :] = prev * 8192 + val_row_i
    meta_v[1:2, :] = last
    meta_copy = pltpu.make_async_copy(meta_v, meta_s, meta_sem)
    meta_copy.start()
    meta_copy.wait()
    q_copy.wait()

    def step(c, carry):
        kv_copy(k_hbm, k_v, k_sem, c).wait()
        kv_copy(v_hbm, v_v, v_sem, c).wait()
        for i in range(PAGES_PER_STEP):
            p = c * PAGES_PER_STEP + i
            code = meta_s[0, p]
            nvalid = jnp.bitwise_and(code, 255) * kvh
            own = jnp.minimum(jnp.bitwise_and(lax.shift_right_logical(code, 8), 31), ns - 1)
            before = jnp.clip(lax.shift_right_logical(code, 13), 0, pages)
            part = pl.ds(pl.multiple_of(p * rows, rows), rows)
            sc = lax.dot_general(q_v[own], k_v[part, :], (((1,), (1,)), ((), ())), preferred_element_type=F32)
            sc = jnp.where(cmod_v[...] < nvalid, sc, NEG)
            top = jnp.max(sc, axis=1, keepdims=True)
            wt = jnp.exp2((sc - top) * scale)
            tot = jnp.sum(wt, axis=1, keepdims=True)
            o = jnp.dot(wt.astype(BF16), v_v[part, :], preferred_element_type=F32)
            mp = mrun[before]
            mb = jnp.broadcast_to(top, (hl, LANES))
            mn = jnp.maximum(mp, mb)
            fa = jnp.exp2((mp - mn) * scale)
            fb = jnp.exp2((mb - mn) * scale)
            mrun[p + 1] = mn
            lrun[p + 1] = fa * lrun[before] + fb * jnp.broadcast_to(tot, (hl, LANES))
            orun[p + 1] = fa * orun[before] + fb * o
        return carry

    lax.fori_loop(0, steps, step, 0)

    lane_h = lax.broadcasted_iota(I32, (hl, LANES), 1)
    mpack = jnp.zeros((hl, LANES), F32)
    lpack = jnp.zeros((hl, LANES), F32)
    for s in range(ns):
        f = jnp.clip(meta_s[1, s], 0, pages)
        ofin[s] = orun[f]
        mpack = jnp.where(lane_h == s, mrun[f], mpack)
        lpack = jnp.where(lane_h == s, lrun[f], lpack)
    both = jnp.concatenate([mpack, lpack, jnp.zeros((LANES - 2 * hl, LANES), F32)], axis=0)
    mlt = jnp.transpose(both)[0:ns, :]
    for ct in range(cores):
        part = mlt[ct * sb : (ct + 1) * sb, :]
        for cx in range(nx):
            s1m[ct, cx] = part if cx == 0 else pltpu.roll(part, LANES - cx * hq, 1)
            for j in range(hq):
                s1o[ct, cx, j] = ofin[ct * sb : (ct + 1) * sb, cx * hq + j, :].astype(BF16)
    r1o[t, x] = s1o[t, x]
    r1m[t, x] = s1m[t, x]

    pl.semaphore_wait(barrier, len(xpeers) + len(order))

    def s1_copies(i, px, pt):
        o = pltpu.make_async_remote_copy(
            src_ref=s1o.at[pt, px], dst_ref=r1o.at[t, x], send_sem=s1s_sem.at[i], recv_sem=s1r_sem.at[t, x],
            device_id=at(px, z, pt), device_id_type=MESH)
        m = pltpu.make_async_remote_copy(
            src_ref=s1m.at[pt, px], dst_ref=r1m.at[t, x], send_sem=s1ms_sem.at[i], recv_sem=s1mr_sem.at[t, x],
            device_id=at(px, z, pt), device_id_type=MESH)
        return m, o

    def s1_arrivals(px, pt):
        o = pltpu.make_async_remote_copy(
            src_ref=s1o.at[pt, px], dst_ref=r1o.at[pt, px], send_sem=s1s_sem.at[0], recv_sem=s1r_sem.at[pt, px],
            device_id=at(px, z, pt), device_id_type=MESH)
        m = pltpu.make_async_remote_copy(
            src_ref=s1m.at[pt, px], dst_ref=r1m.at[pt, px], send_sem=s1ms_sem.at[0], recv_sem=s1mr_sem.at[pt, px],
            device_id=at(px, z, pt), device_id_type=MESH)
        return m, o

    for i, (px, pt) in enumerate(xpeers):
        for copy in s1_copies(i, px, pt):
            copy.start()

    w_copy.wait()
    w_send = pltpu.make_async_remote_copy(
        src_ref=w_v.at[t], dst_ref=w_v.at[t], send_sem=ws_sem, recv_sem=wr_sem,
        device_id=at(x, z, (t + 1) % cores), device_id_type=MESH)
    w_recv = pltpu.make_async_remote_copy(
        src_ref=w_v.at[t], dst_ref=w_v.at[(t + 1) % cores], send_sem=ws_sem, recv_sem=wr_sem,
        device_id=at(x, z, (t + 1) % cores), device_id_type=MESH)
    w_send.start()

    for px, pt in xpeers:
        for copy in s1_arrivals(px, pt):
            copy.wait_recv()

    lane_s = lax.broadcasted_iota(I32, (sb, LANES), 1)
    tops, sums = [], []
    for ct in range(cores):
        ml = [r1m[ct, cx] for cx in range(nx)]
        top = functools.reduce(jnp.maximum, ml)
        fs = [jnp.exp2((m - top) * scale) for m in ml]
        tot = functools.reduce(jnp.add, [f * pltpu.roll(m, LANES - hl, 1) for f, m in zip(fs, ml)])
        tops.append(top)
        sums.append(tot)
        for j in range(hq):
            num = functools.reduce(
                jnp.add,
                [jnp.broadcast_to(fs[cx][:, j : j + 1], (sb, hd)) * r1o[ct, cx, j].astype(F32) for cx in range(nx)])
            s2o[ct * hq + j] = num.astype(BF16)
    mm = jnp.where(lane_s < hq, tops[0], pltpu.roll(tops[1], hq, 1))
    ll = jnp.where(lane_s < hq, sums[0], pltpu.roll(sums[1], hq, 1))
    both = jnp.concatenate([mm, ll, jnp.zeros((LANES - 2 * sb, LANES), F32)], axis=0)
    s2m[...] = jnp.transpose(both)[0:nz, :].reshape(nz, 1, LANES)
    r2o[z] = s2o[z]
    r2m[z] = s2m[z]

    def s2_copies(d, dst_z, src_z, slot_z):
        o = pltpu.make_async_remote_copy(
            src_ref=s2o.at[dst_z], dst_ref=r2o.at[slot_z], send_sem=s2s_sem.at[d], recv_sem=s2r_sem.at[slot_z],
            device_id=at(x, dst_z, t), device_id_type=MESH)
        m = pltpu.make_async_remote_copy(
            src_ref=s2m.at[dst_z], dst_ref=r2m.at[slot_z], send_sem=s2ms_sem.at[d], recv_sem=s2mr_sem.at[slot_z],
            device_id=at(x, dst_z, t), device_id_type=MESH)
        return m, o

    for d in order:
        for copy in s2_copies(d, (z + d) % nz, z, z):
            copy.start()
    for d in reversed(order):
        pz = (z + d) % nz
        for copy in s2_copies(d, pz, pz, pz):
            copy.wait_recv()

    ml = r2m[...].reshape(nz, LANES)
    top = jnp.max(ml, axis=0, keepdims=True)
    f = jnp.exp2((ml - top) * scale)
    den = jnp.sum(f * pltpu.roll(ml, LANES - sb, 1), axis=0, keepdims=True)
    lane_z = lax.broadcasted_iota(I32, (nz, LANES), 1)
    f = jnp.where(lane_z < sb, f / den, 0.0)
    ft = jnp.transpose(jnp.concatenate([f, jnp.zeros((LANES - nz, LANES), F32)], axis=0))[0:sb, :]
    att = functools.reduce(
        jnp.add, [jnp.broadcast_to(ft[:, i : i + 1], (sb, hd)) * r2o[i].astype(F32) for i in range(nz)])
    g_v[x, z] = att.astype(BF16)

    def gz_copy(d, pz, slot):
        return pltpu.make_async_remote_copy(
            src_ref=g_v.at[x, z], dst_ref=g_v.at[x, slot], send_sem=gzs_sem.at[d], recv_sem=gzr_sem.at[slot],
            device_id=at(x, pz, t), device_id_type=MESH)

    def gx_copy(dx, slot_x, slot):
        return pltpu.make_async_remote_copy(
            src_ref=g_v.at[x, slot], dst_ref=g_v.at[slot_x, slot], send_sem=gxs_sem.at[dx, slot],
            recv_sem=gxr_sem.at[slot_x, slot], device_id=at((x + dx) % nx, z, t), device_id_type=MESH)

    for d in order:
        gz_copy(d, (z + d) % nz, z).start()
    for dx in range(1, nx):
        gx_copy(dx, x, z).start()
    for d in reversed(order):
        pz = (z + d) % nz
        gz_copy(d, pz, pz).wait_recv()
        for dx in range(1, nx):
            gx_copy(dx, x, pz).start()
    w_recv.wait_recv()
    for dx in range(1, nx):
        for d in range(nz):
            gx_copy(dx, (x + dx) % nx, d).wait_recv()

    out = jnp.zeros((sb, hd), F32)
    for ct in range(cores):
        for cx in range(nx):
            for j in range(0, hq, 2):
                lhs = jnp.concatenate([g_v[cx, ct * hq + j], g_v[cx, ct * hq + j + 1]], axis=1)
                first = (cx * hq + j) * hd
                out = out + jnp.dot(lhs, w_v[ct, first : first + 2 * hd, :], preferred_element_type=F32)
    out_ref[...] = out.astype(out_ref.dtype)

    w_send.wait_send()
    for i, (px, pt) in enumerate(xpeers):
        for copy in s1_copies(i, px, pt):
            copy.wait_send()
    for d in order:
        for copy in s2_copies(d, (z + d) % nz, z, z):
            copy.wait_send()
        gz_copy(d, (z + d) % nz, z).wait_send()
    for dx in range(1, nx):
        for d in range(nz):
            gx_copy(dx, x, d).wait_send()


def body(query, key_cache, value_cache, lengths, page_order, out_weight):
    pages, page_len, kvh, hd = key_cache.shape
    ns, hl = query.shape[0], query.shape[1]
    cores = lax.axis_size("tensor")
    nz = ns
    nx = lax.axis_size("seq") // nz
    hq = hl // nx
    sb = ns // cores
    rows = page_len * kvh
    pr = page_order.shape[0] // LANES
    wr, wc = out_weight.shape
    dims = (nx, nz, pages, page_len, kvh, ns, hl, hd, cores)
    steps = pages // PAGES_PER_STEP
    nxp = nx * cores - 1
    dma = pltpu.SemaphoreType.DMA
    return pl.pallas_call(
        functools.partial(kernel, dims),
        out_shape=jax.ShapeDtypeStruct((sb, wc), BF16),
        in_specs=[pl.BlockSpec(memory_space=pltpu.SMEM)] + [pl.BlockSpec(memory_space=pl.ANY)] * 5,
        out_specs=pl.BlockSpec(memory_space=pltpu.VMEM),
        scratch_shapes=[
            pltpu.VMEM((ns, hl, hd), BF16),
            pltpu.VMEM((pages * rows, hd), BF16),
            pltpu.VMEM((pages * rows, hd), BF16),
            pltpu.VMEM((pr, LANES), I32),
            pltpu.VMEM((cores, wr, wc), BF16),
            pltpu.VMEM((pr, LANES), F32),
            pltpu.VMEM((8, LANES), I32),
            pltpu.SMEM((8, LANES), I32),
            pltpu.VMEM((hl, rows), I32),
            pltpu.VMEM((pages + 1, hl, LANES), F32),
            pltpu.VMEM((pages + 1, hl, LANES), F32),
            pltpu.VMEM((pages + 1, hl, hd), F32),
            pltpu.VMEM((ns, hl, hd), F32),
            pltpu.VMEM((cores, nx, hq, sb, hd), BF16),
            pltpu.VMEM((cores, nx, sb, LANES), F32),
            pltpu.VMEM((cores, nx, hq, sb, hd), BF16),
            pltpu.VMEM((cores, nx, sb, LANES), F32),
            pltpu.VMEM((nz, sb, hd), BF16),
            pltpu.VMEM((nz, 1, LANES), F32),
            pltpu.VMEM((nz, sb, hd), BF16),
            pltpu.VMEM((nz, 1, LANES), F32),
            pltpu.VMEM((nx, nz, sb, hd), BF16),
            pltpu.VMEM((sb, LANES), F32),
            dma, dma((steps,)), dma((steps,)), dma, dma, dma,
            dma, dma, dma((nxp,)), dma((cores, nx)), dma((nxp,)), dma((cores, nx)),
            dma((nz,)), dma((nz,)), dma((nz,)), dma((nz,)), dma((nz,)), dma((nz,)), dma((nx, nz)), dma((nx, nz)),
        ],
        compiler_params=pltpu.CompilerParams(collective_id=0, has_side_effects=True),
        name="paged_decode",
    )(
        lengths, query, key_cache.reshape(pages * rows, hd), value_cache.reshape(pages * rows, hd),
        page_order.reshape(pr, LANES), out_weight)


def solution(mesh):
    in_specs = (
        P("group", "tensor", None),
        P(("group", "seq"), None, "tensor", None),
        P(("group", "seq"), None, "tensor", None),
        P("group"),
        P("group"),
        P("tensor", "seq"),
    )
    out_specs = P(("group", "tensor"), "seq")
    return jax.shard_map(body, mesh=mesh, in_specs=in_specs, out_specs=out_specs, check_vma=False)
```

```python
import functools
import math

import jax
import jax.numpy as jnp
from jax import lax
from jax.experimental import pallas as pl
from jax.experimental.pallas import tpu as pltpu
from jax.sharding import PartitionSpec as P

MESH = pl.DeviceIdType.MESH
F32 = jnp.float32
BF16 = jnp.bfloat16
I32 = jnp.int32
LANES = 128
NEG = -1e30
PAGES_PER_STEP = 8


def kernel(
    dims,
    len_s, q_hbm, k_hbm, v_hbm, po_hbm, w_hbm, out_ref,
    q_v, k_v, v_v, po_v, w_v, val_v, meta_v, meta_s, cmod_v,
    wt_v, mtop, ltot, mrun, lrun, orun, ofin,
    s1o, s1m, r1o, r1m, s2o, s2m, r2o, r2m, g_v,
    q_sem, k_sem, v_sem, po_sem, w_sem, meta_sem,
    ws_sem, wr_sem, s1s_sem, s1r_sem, s1ms_sem, s1mr_sem,
    s2s_sem, s2r_sem, s2ms_sem, s2mr_sem, gd_sem, gz_sem, gx_sem, gr_sem,
):
    nx, nz, pages, page_len, kvh, ns, hl, hd, cores = dims
    rows = page_len * kvh
    hq = hl // nx
    sb = ns // cores
    group_size = hl // kvh
    scale = math.log2(math.e) / math.sqrt(hd)
    me = lax.axis_index("seq")
    t = lax.axis_index("tensor")
    x = me // nz
    z = me % nz
    steps = pages // PAGES_PER_STEP
    spots = (nz - 1, 0)

    def at(px, pz, pt):
        return {"seq": px * nz + pz, "tensor": pt}

    def remote(src, dst, send, recv, to):
        return pltpu.make_async_remote_copy(
            src_ref=src, dst_ref=dst, send_sem=send, recv_sem=recv, device_id=to, device_id_type=MESH)

    po_copy = pltpu.make_async_copy(po_hbm, po_v, po_sem)
    po_copy.start()
    q_copy = pltpu.make_async_copy(q_hbm, q_v, q_sem)
    q_copy.start()
    step_rows = PAGES_PER_STEP * rows

    def kv_copy(src, dst, sem, c):
        part = pl.ds(c * step_rows, step_rows)
        return pltpu.make_async_copy(src.at[part], dst.at[part], sem.at[c])

    for c in range(steps):
        kv_copy(k_hbm, k_v, k_sem, c).start()
    for c in range(steps):
        kv_copy(v_hbm, v_v, v_sem, c).start()
    w_copy = pltpu.make_async_copy(w_hbm, w_v.at[t], w_sem)
    w_copy.start()

    xpeers = []
    for dx in range(nx):
        for dt in range(cores):
            if dx or dt:
                xpeers.append(((x + dx) % nx, (t + dt) % cores))
    is_spot = (z == spots[0]) | (z == spots[1])
    barrier = pltpu.get_barrier_semaphore()

    def greet(px, pz, pt):
        pl.semaphore_signal(barrier, inc=1, device_id=at(px, pz, pt), device_id_type=MESH)

    for px, pt in xpeers:
        greet(px, z, pt)
    for o in range(cores):
        @pl.when(z != spots[o])
        def _():
            greet(x, spots[o], t)

        @pl.when(z == spots[o])
        def _():
            for pz in range(nz):
                if pz not in spots:
                    greet(x, pz, t)
            for dx in range(1, nx):
                greet((x + dx) % nx, spots[1 - o], t)

    lens = [len_s[s] for s in range(ns)]
    starts = []
    run = jnp.int32(0)
    for s in range(ns):
        starts.append(run)
        run = run + lax.shift_right_logical(lens[s] + (page_len - 1), int(math.log2(page_len)))
    pr = po_v.shape[0]
    rank = lax.broadcasted_iota(I32, (pr, LANES), 0) * LANES + lax.broadcasted_iota(I32, (pr, LANES), 1)
    owner = jnp.zeros((pr, LANES), I32)
    end = jnp.full((pr, LANES), lens[0], I32)
    for s in range(1, ns):
        past = rank >= starts[s]
        owner = jnp.where(past, s, owner)
        end = jnp.where(past, lens[s] + starts[s] * page_len, end)
    valid = jnp.clip(end - rank * page_len, 0, page_len)
    owner = jnp.where(valid > 0, owner, ns)
    val_v[...] = (owner * 256 + valid).astype(F32)

    cl = lax.broadcasted_iota(I32, (hl, rows), 1)
    hr = lax.broadcasted_iota(I32, (hl, rows), 0)
    cmod_v[...] = jnp.where(cl % kvh == hr // group_size, cl, 1 << 20)
    mrun[0] = jnp.full((hl, LANES), NEG, F32)
    lrun[0] = jnp.zeros((hl, LANES), F32)
    orun[0] = jnp.zeros((hl, hd), F32)

    po_copy.wait()
    ids = lax.broadcasted_iota(I32, (pages, LANES), 0) + me * pages
    acc = jnp.zeros((pages, LANES), F32)
    for i in range(pr):
        hit = jnp.broadcast_to(po_v[i : i + 1, :], (pages, LANES)) == ids
        acc = acc + jnp.where(hit, jnp.broadcast_to(val_v[i : i + 1, :], (pages, LANES)), 0.0)
    val_col = jnp.broadcast_to(jnp.sum(acc, axis=1, keepdims=True), (pages, LANES))
    pad = jnp.concatenate([val_col, jnp.zeros((LANES - pages, LANES), F32)], axis=0)
    val_row = jnp.transpose(pad)[0:1, :]
    own_col = lax.shift_right_logical(val_col.astype(I32), 8)
    val_row_i = val_row.astype(I32)
    own_row = lax.shift_right_logical(val_row_i, 8)
    prow = lax.broadcasted_iota(I32, (pages, LANES), 0)
    lane = lax.broadcasted_iota(I32, (pages, LANES), 1)
    same = (own_col == jnp.broadcast_to(own_row, (pages, LANES))) & (prow < lane)
    prev = jnp.max(jnp.where(same, (prow + 1).astype(F32), 0.0), axis=0, keepdims=True).astype(I32)
    last = jnp.max(jnp.where(own_col == lane, (prow + 1).astype(F32), 0.0), axis=0, keepdims=True).astype(I32)
    meta_v[0:1, :] = prev * 8192 + val_row_i
    meta_v[1:2, :] = last
    meta_copy = pltpu.make_async_copy(meta_v, meta_s, meta_sem)
    meta_copy.start()
    meta_copy.wait()
    q_copy.wait()

    def page_part(p):
        return pl.ds(pl.multiple_of(p * rows, rows), rows)

    def score_step(c, carry):
        kv_copy(k_hbm, k_v, k_sem, c).wait()
        for i in range(PAGES_PER_STEP):
            p = c * PAGES_PER_STEP + i
            code = meta_s[0, p]
            nvalid = jnp.bitwise_and(code, 255) * kvh
            own = jnp.minimum(jnp.bitwise_and(lax.shift_right_logical(code, 8), 31), ns - 1)
            before = jnp.clip(lax.shift_right_logical(code, 13), 0, pages)
            sc = lax.dot_general(
                q_v[own], k_v[page_part(p), :], (((1,), (1,)), ((), ())), preferred_element_type=F32)
            sc = jnp.where(cmod_v[...] < nvalid, sc, NEG)
            top = jnp.max(sc, axis=1, keepdims=True)
            wt = jnp.exp2((sc - top) * scale)
            wt_v[p] = wt.astype(BF16)
            top = jnp.broadcast_to(top, (hl, LANES))
            mtop[p] = top
            ltot[p] = jnp.broadcast_to(jnp.sum(wt, axis=1, keepdims=True), (hl, LANES))
            mrun[p + 1] = jnp.maximum(mrun[before], top)
        return carry

    lax.fori_loop(0, steps, score_step, 0)

    def value_step(c, carry):
        kv_copy(v_hbm, v_v, v_sem, c).wait()
        for i in range(PAGES_PER_STEP):
            p = c * PAGES_PER_STEP + i
            code = meta_s[0, p]
            own = jnp.bitwise_and(lax.shift_right_logical(code, 8), 31)
            before = jnp.clip(lax.shift_right_logical(code, 13), 0, pages)
            final = jnp.clip(meta_s[1, own], 0, pages)
            o = jnp.dot(wt_v[p], v_v[page_part(p), :], preferred_element_type=F32)
            fb = jnp.exp2((mtop[p] - mrun[final]) * scale)
            lrun[p + 1] = lrun[before] + fb * ltot[p]
            orun[p + 1] = orun[before] + fb * o
        return carry

    lax.fori_loop(0, steps, value_step, 0)

    lane_h = lax.broadcasted_iota(I32, (hl, LANES), 1)
    mpack = jnp.zeros((hl, LANES), F32)
    lpack = jnp.zeros((hl, LANES), F32)
    for s in range(ns):
        f = jnp.clip(meta_s[1, s], 0, pages)
        ofin[s] = orun[f]
        mpack = jnp.where(lane_h == s, mrun[f], mpack)
        lpack = jnp.where(lane_h == s, lrun[f], lpack)
    both = jnp.concatenate([mpack, lpack, jnp.zeros((LANES - 2 * hl, LANES), F32)], axis=0)
    mlt = jnp.transpose(both)[0:ns, :]
    for ct in range(cores):
        part = mlt[ct * sb : (ct + 1) * sb, :]
        for cx in range(nx):
            s1m[ct, cx] = part if cx == 0 else pltpu.roll(part, LANES - cx * hq, 1)
            for j in range(hq):
                s1o[ct, cx, j] = ofin[ct * sb : (ct + 1) * sb, cx * hq + j, :].astype(BF16)
    r1o[t, x] = s1o[t, x]
    r1m[t, x] = s1m[t, x]

    pl.semaphore_wait(barrier, len(xpeers) + jnp.where(is_spot, nz - 1 + nx - 1, cores))

    def s1_copies(i, px, pt, ft, fx):
        to = at(px, z, pt)
        return (
            remote(s1m.at[pt, px], r1m.at[ft, fx], s1ms_sem.at[i], s1mr_sem.at[ft, fx], to),
            remote(s1o.at[pt, px], r1o.at[ft, fx], s1s_sem.at[i], s1r_sem.at[ft, fx], to))

    for i, (px, pt) in enumerate(xpeers):
        for copy in s1_copies(i, px, pt, t, x):
            copy.start()

    w_copy.wait()
    w_send = remote(w_v.at[t], w_v.at[t], ws_sem, wr_sem, at(x, z, (t + 1) % cores))
    w_recv = remote(w_v.at[t], w_v.at[(t + 1) % cores], ws_sem, wr_sem, at(x, z, (t + 1) % cores))
    w_send.start()

    for i, (px, pt) in enumerate(xpeers):
        for copy in s1_copies(i, px, pt, pt, px):
            copy.wait_recv()

    lane_s = lax.broadcasted_iota(I32, (sb, LANES), 1)

    def merged(ml):
        top = functools.reduce(jnp.maximum, ml)
        fs = [jnp.exp2((m - top) * scale) for m in ml]
        tot = functools.reduce(jnp.add, [f * pltpu.roll(m, LANES - hl, 1) for f, m in zip(fs, ml)])
        return top, fs, tot

    def s2_copies(o, slot):
        to = at(x, spots[o], t)
        return (
            remote(s2m.at[o], r2m.at[slot], s2ms_sem.at[o], s2mr_sem.at[slot], to),
            remote(s2o.at[o], r2o.at[slot], s2s_sem.at[o], s2r_sem.at[slot], to))

    for o in reversed(range(cores)):
        top, fs, tot = merged([r1m[o, cx] for cx in range(nx)])
        s2m[o] = jnp.where(lane_s < hq, top, pltpu.roll(tot, hl, 1))
        for j in range(hq):
            num = functools.reduce(
                jnp.add,
                [jnp.broadcast_to(fs[cx][:, j : j + 1], (sb, hd)) * r1o[o, cx, j].astype(F32) for cx in range(nx)])
            s2o[o, j] = num.astype(BF16)

        @pl.when(z != spots[o])
        def _():
            for copy in s2_copies(o, z):
                copy.start()

        @pl.when(z == spots[o])
        def _():
            r2m[z] = s2m[o]
            r2o[z] = s2o[o]

    def direct(dx):
        return remote(
            g_v.at[x, 0], g_v.at[x, 0], gd_sem.at[dx], gr_sem.at[x, 0], at((x + dx) % nx, spots[1], t))

    def along_z(o, pz):
        return remote(g_v.at[x, o], g_v.at[x, o], gz_sem.at[pz], gr_sem.at[x, o], at(x, pz, t))

    def along_x(o, dx):
        return remote(
            g_v.at[x, o], g_v.at[x, o], gx_sem.at[o, dx], gr_sem.at[x, o], at((x + dx) % nx, z, t))

    def arrival(o, sx):
        return remote(g_v.at[sx, o], g_v.at[sx, o], gd_sem.at[0], gr_sem.at[sx, o], at(x, z, (t + 1) % cores))

    xorder = [d for d in range(nx) if d]
    for o in reversed(range(cores)):
        zorder = [(spots[o] + d) % nz for d in range(1, nz)]
        if o == 0:
            zorder = [pz for pz in zorder if pz != spots[1]]

        @pl.when(z == spots[o])
        def _():
            for pz in range(nz):
                if pz != spots[o]:
                    for copy in (
                        remote(s2m.at[o], r2m.at[pz], s2ms_sem.at[o], s2mr_sem.at[pz], at(x, pz, t)),
                        remote(s2o.at[o], r2o.at[pz], s2s_sem.at[o], s2r_sem.at[pz], at(x, pz, t))):
                        copy.wait_recv()
            top, fs, tot = merged([r2m[i] for i in range(nz)])
            inv = jnp.where(lane_s < hq, 1.0 / tot, 0.0)
            fs = [f * inv for f in fs]
            for j in range(hq):
                att = functools.reduce(
                    jnp.add,
                    [jnp.broadcast_to(fs[i][:, j : j + 1], (sb, hd)) * r2o[i, j].astype(F32) for i in range(nz)])
                g_v[x, o, j] = att.astype(BF16)
            if o == 0:
                for dx in xorder + [0]:
                    direct(dx).start()
            else:
                for dx in xorder:
                    along_x(o, dx).start()
            for pz in zorder:
                along_z(o, pz).start()
            if o == 0:
                for dx in xorder:
                    along_x(o, dx).start()

    for o in reversed(range(cores)):
        @pl.when((z != spots[o]) & ((z != spots[1]) | (o == 1)))
        def _():
            arrival(o, x).wait_recv()
            for dx in xorder:
                along_x(o, dx).start()

    @pl.when(z == spots[1])
    def _():
        arrival(0, x).wait_recv()

    w_recv.wait_recv()

    out = jnp.zeros((sb, hd), F32)
    for dx in [0] + xorder:
        sx = (x + dx) % nx
        for o in reversed(range(cores)):
            if dx:
                arrival(o, sx).wait_recv()
            for j in range(0, hq, 2):
                lhs = jnp.concatenate([g_v[sx, o, j], g_v[sx, o, j + 1]], axis=1)
                first = pl.multiple_of((sx * hq + j) * hd, 2 * hd)
                out = out + jnp.dot(lhs, w_v[o, pl.ds(first, 2 * hd), :], preferred_element_type=F32)
    out_ref[...] = out.astype(out_ref.dtype)

    w_send.wait_send()
    for i, (px, pt) in enumerate(xpeers):
        for copy in s1_copies(i, px, pt, t, x):
            copy.wait_send()
    for o in range(cores):
        @pl.when(z != spots[o])
        def _():
            for copy in s2_copies(o, z):
                copy.wait_send()

        @pl.when(z == spots[o])
        def _():
            for pz in range(nz):
                if pz != spots[o] and not (o == 0 and pz == spots[1]):
                    along_z(o, pz).wait_send()
            if o == 0:
                for dx in range(nx):
                    direct(dx).wait_send()

        @pl.when((z != spots[1]) | (o == 1))
        def _():
            for dx in xorder:
                along_x(o, dx).wait_send()


def body(query, key_cache, value_cache, lengths, page_order, out_weight):
    pages, page_len, kvh, hd = key_cache.shape
    ns, hl = query.shape[0], query.shape[1]
    cores = lax.axis_size("tensor")
    nz = ns
    nx = lax.axis_size("seq") // nz
    hq = hl // nx
    sb = ns // cores
    rows = page_len * kvh
    pr = page_order.shape[0] // LANES
    wr, wc = out_weight.shape
    dims = (nx, nz, pages, page_len, kvh, ns, hl, hd, cores)
    steps = pages // PAGES_PER_STEP
    nxp = nx * cores - 1
    dma = pltpu.SemaphoreType.DMA
    return pl.pallas_call(
        functools.partial(kernel, dims),
        out_shape=jax.ShapeDtypeStruct((sb, wc), BF16),
        in_specs=[pl.BlockSpec(memory_space=pltpu.SMEM)] + [pl.BlockSpec(memory_space=pl.ANY)] * 5,
        out_specs=pl.BlockSpec(memory_space=pltpu.VMEM),
        scratch_shapes=[
            pltpu.VMEM((ns, hl, hd), BF16),
            pltpu.VMEM((pages * rows, hd), BF16),
            pltpu.VMEM((pages * rows, hd), BF16),
            pltpu.VMEM((pr, LANES), I32),
            pltpu.VMEM((cores, wr, wc), BF16),
            pltpu.VMEM((pr, LANES), F32),
            pltpu.VMEM((8, LANES), I32),
            pltpu.SMEM((8, LANES), I32),
            pltpu.VMEM((hl, rows), I32),
            pltpu.VMEM((pages, hl, rows), BF16),
            pltpu.VMEM((pages, hl, LANES), F32),
            pltpu.VMEM((pages, hl, LANES), F32),
            pltpu.VMEM((pages + 1, hl, LANES), F32),
            pltpu.VMEM((pages + 1, hl, LANES), F32),
            pltpu.VMEM((pages + 1, hl, hd), F32),
            pltpu.VMEM((ns, hl, hd), F32),
            pltpu.VMEM((cores, nx, hq, sb, hd), BF16),
            pltpu.VMEM((cores, nx, sb, LANES), F32),
            pltpu.VMEM((cores, nx, hq, sb, hd), BF16),
            pltpu.VMEM((cores, nx, sb, LANES), F32),
            pltpu.VMEM((cores, hq, sb, hd), BF16),
            pltpu.VMEM((cores, sb, LANES), F32),
            pltpu.VMEM((nz, hq, sb, hd), BF16),
            pltpu.VMEM((nz, sb, LANES), F32),
            pltpu.VMEM((nx, cores, hq, sb, hd), BF16),
            dma, dma((steps,)), dma((steps,)), dma, dma, dma,
            dma, dma, dma((nxp,)), dma((cores, nx)), dma((nxp,)), dma((cores, nx)),
            dma((cores,)), dma((nz,)), dma((cores,)), dma((nz,)),
            dma((nx,)), dma((nz,)), dma((cores, nx)), dma((nx, cores)),
        ],
        compiler_params=pltpu.CompilerParams(collective_id=0, has_side_effects=True),
        name="paged_decode",
    )(
        lengths, query, key_cache.reshape(pages * rows, hd), value_cache.reshape(pages * rows, hd),
        page_order.reshape(pr, LANES), out_weight)


def solution(mesh):
    in_specs = (
        P("group", "tensor", None),
        P(("group", "seq"), None, "tensor", None),
        P(("group", "seq"), None, "tensor", None),
        P("group"),
        P("group"),
        P("tensor", "seq"),
    )
    out_specs = P(("group", "tensor"), "seq")
    return jax.shard_map(body, mesh=mesh, in_specs=in_specs, out_specs=out_specs, check_vma=False)
```

```python
import functools
import math

import jax
import jax.numpy as jnp
from jax import lax
from jax.experimental import pallas as pl
from jax.experimental.pallas import tpu as pltpu
from jax.sharding import PartitionSpec as P

MESH = pl.DeviceIdType.MESH
F32 = jnp.float32
BF16 = jnp.bfloat16
I32 = jnp.int32
LANES = 128
NEG = -1e30
PAGES_PER_STEP = 8


def kernel(
    dims,
    len_hbm, q_hbm, k_hbm, v_hbm, po_hbm, w_hbm, out_ref,
    len_s, q_v, k_v, v_v, po_v, w_v, val_v, meta_v, meta_s, cmod_v,
    wt_v, mtop, ltot, mrun, lrun, orun, ofin, s1, r1, s2, r2, s1m, r1m, s2m, r2m, g_v,
    len_sem, q_sem, k_sem, v_sem, po_sem, w_sem, meta_sem, ws_sem, wr_sem,
    s1s_sem, s1r_sem, s2s_sem, s2r_sem, m1s_sem, m1r_sem, m2s_sem, m2r_sem, gzs_sem, gxs_sem, own_sem, peer_sem,
):
    nx, nz, pages, page_len, kvh, ns, hl, hd, cores = dims
    rows = page_len * kvh
    hq = hl // nx
    sb = ns // cores
    group_size = hl // kvh
    scale = math.log2(math.e) / math.sqrt(hd)
    me = lax.axis_index("seq")
    t = lax.axis_index("tensor")
    x = me // nz
    z = me % nz
    steps = pages // PAGES_PER_STEP
    spots = (1, 0)

    def at(px, pz, pt):
        return {"seq": px * nz + pz, "tensor": pt}

    def remote(src, dst, send, recv, to):
        return pltpu.make_async_remote_copy(
            src_ref=src, dst_ref=dst, send_sem=send, recv_sem=recv, device_id=to, device_id_type=MESH)

    len_copy = pltpu.make_async_copy(len_hbm, len_s, len_sem)
    len_copy.start()
    po_copy = pltpu.make_async_copy(po_hbm, po_v, po_sem)
    po_copy.start()
    q_copy = pltpu.make_async_copy(q_hbm, q_v, q_sem)
    q_copy.start()

    xpeers = []
    for dx in range(nx):
        for dt in range(cores):
            if dx or dt:
                xpeers.append(((x + dx) % nx, (t + dt) % cores))
    barrier = pltpu.get_barrier_semaphore()

    def greet(px, pz, pt):
        pl.semaphore_signal(barrier, inc=1, device_id=at(px, pz, pt), device_id_type=MESH)

    for px, pt in xpeers:
        greet(px, z, pt)

    step_rows = PAGES_PER_STEP * rows

    def kv_copy(src, dst, sem, c):
        part = pl.ds(c * step_rows, step_rows)
        return pltpu.make_async_copy(src.at[part], dst.at[part], sem.at[c])

    for c in range(steps):
        kv_copy(k_hbm, k_v, k_sem, c).start()
    for c in range(steps):
        kv_copy(v_hbm, v_v, v_sem, c).start()
    w_copy = pltpu.make_async_copy(w_hbm, w_v.at[t], w_sem)
    w_copy.start()

    for o in range(cores):
        @pl.when(z == spots[o])
        def _():
            for d in range(1, nz):
                greet(x, (z + d) % nz, t)
            if o == 1:
                for dx in range(1, nx):
                    greet((x + dx) % nx, spots[0], t)

    cl = lax.broadcasted_iota(I32, (hl, rows), 1)
    hr = lax.broadcasted_iota(I32, (hl, rows), 0)
    cmod_v[...] = jnp.where(cl % kvh == hr // group_size, cl, 1 << 20)
    mrun[0] = jnp.full((hl, LANES), NEG, F32)
    lrun[0] = jnp.zeros((hl, LANES), F32)
    orun[0] = jnp.zeros((hl, hd), F32)

    len_copy.wait()
    lens = [len_s[s] for s in range(ns)]
    starts = []
    run = jnp.int32(0)
    for s in range(ns):
        starts.append(run)
        run = run + lax.shift_right_logical(lens[s] + (page_len - 1), int(math.log2(page_len)))
    pr = po_v.shape[0]
    rank = lax.broadcasted_iota(I32, (pr, LANES), 0) * LANES + lax.broadcasted_iota(I32, (pr, LANES), 1)
    owner = jnp.zeros((pr, LANES), I32)
    end = jnp.full((pr, LANES), lens[0], I32)
    for s in range(1, ns):
        past = rank >= starts[s]
        owner = jnp.where(past, s, owner)
        end = jnp.where(past, lens[s] + starts[s] * page_len, end)
    valid = jnp.clip(end - rank * page_len, 0, page_len)
    owner = jnp.where(valid > 0, owner, ns)
    val_v[...] = (owner * 256 + valid).astype(F32)

    po_copy.wait()
    ids = lax.broadcasted_iota(I32, (pages, LANES), 0) + me * pages
    acc = jnp.zeros((pages, LANES), F32)
    for i in range(pr):
        hit = jnp.broadcast_to(po_v[i : i + 1, :], (pages, LANES)) == ids
        acc = acc + jnp.where(hit, jnp.broadcast_to(val_v[i : i + 1, :], (pages, LANES)), 0.0)
    val_col = jnp.broadcast_to(jnp.sum(acc, axis=1, keepdims=True), (pages, LANES))
    pad = jnp.concatenate([val_col, jnp.zeros((LANES - pages, LANES), F32)], axis=0)
    val_row = jnp.transpose(pad)[0:1, :]
    own_col = lax.shift_right_logical(val_col.astype(I32), 8)
    val_row_i = val_row.astype(I32)
    own_row = lax.shift_right_logical(val_row_i, 8)
    prow = lax.broadcasted_iota(I32, (pages, LANES), 0)
    lane = lax.broadcasted_iota(I32, (pages, LANES), 1)
    same = (own_col == jnp.broadcast_to(own_row, (pages, LANES))) & (prow < lane)
    prev = jnp.max(jnp.where(same, (prow + 1).astype(F32), 0.0), axis=0, keepdims=True).astype(I32)
    last = jnp.max(jnp.where(own_col == lane, (prow + 1).astype(F32), 0.0), axis=0, keepdims=True).astype(I32)
    meta_v[0:1, :] = prev * 8192 + val_row_i
    meta_v[1:2, :] = last
    meta_copy = pltpu.make_async_copy(meta_v, meta_s, meta_sem)
    meta_copy.start()
    meta_copy.wait()
    q_copy.wait()

    def page_part(p):
        return pl.ds(pl.multiple_of(p * rows, rows), rows)

    def score_step(c, carry):
        kv_copy(k_hbm, k_v, k_sem, c).wait()
        for i in range(PAGES_PER_STEP):
            p = c * PAGES_PER_STEP + i
            code = meta_s[0, p]
            nvalid = jnp.bitwise_and(code, 255) * kvh
            own = jnp.minimum(jnp.bitwise_and(lax.shift_right_logical(code, 8), 31), ns - 1)
            before = jnp.clip(lax.shift_right_logical(code, 13), 0, pages)
            sc = lax.dot_general(
                q_v[own], k_v[page_part(p), :], (((1,), (1,)), ((), ())), preferred_element_type=F32)
            sc = jnp.where(cmod_v[...] < nvalid, sc, NEG)
            top = jnp.max(sc, axis=1, keepdims=True)
            wt = jnp.exp2((sc - top) * scale)
            wt_v[p] = wt.astype(BF16)
            top = jnp.broadcast_to(top, (hl, LANES))
            mtop[p] = top
            ltot[p] = jnp.broadcast_to(jnp.sum(wt, axis=1, keepdims=True), (hl, LANES))
            mrun[p + 1] = jnp.maximum(mrun[before], top)
        return carry

    lax.fori_loop(0, steps, score_step, 0)

    def value_step(c, carry):
        kv_copy(v_hbm, v_v, v_sem, c).wait()
        for i in range(PAGES_PER_STEP):
            p = c * PAGES_PER_STEP + i
            code = meta_s[0, p]
            own = jnp.bitwise_and(lax.shift_right_logical(code, 8), 31)
            before = jnp.clip(lax.shift_right_logical(code, 13), 0, pages)
            final = jnp.clip(meta_s[1, own], 0, pages)
            o = jnp.dot(wt_v[p], v_v[page_part(p), :], preferred_element_type=F32)
            fb = jnp.exp2((mtop[p] - mrun[final]) * scale)
            lrun[p + 1] = lrun[before] + fb * ltot[p]
            orun[p + 1] = orun[before] + fb * o
        return carry

    lax.fori_loop(0, steps, value_step, 0)

    lane_h = lax.broadcasted_iota(I32, (hl, LANES), 1)
    mpack = jnp.zeros((hl, LANES), F32)
    lpack = jnp.zeros((hl, LANES), F32)
    for s in range(ns):
        f = jnp.clip(meta_s[1, s], 0, pages)
        ofin[s] = orun[f]
        mpack = jnp.where(lane_h == s, mrun[f], mpack)
        lpack = jnp.where(lane_h == s, lrun[f], lpack)
    gap = jnp.zeros((LANES // 2 - hl, LANES), F32)
    mlt = jnp.transpose(jnp.concatenate([mpack, gap, lpack, gap], axis=0))[0:ns, :]
    lane_s = lax.broadcasted_iota(I32, (sb, LANES), 1)
    half = LANES // 2
    for ct in range(cores):
        part = mlt[ct * sb : (ct + 1) * sb, :]
        for cx in range(nx):
            s1m[ct * nx + cx] = part if cx == 0 else pltpu.roll(part, LANES - cx * hq, 1)
            for j in range(hq):
                s1[ct * nx + cx, j] = ofin[ct * sb : (ct + 1) * sb, cx * hq + j, :].astype(BF16)
    r1[t * nx + x] = s1[t * nx + x]
    r1m[t * nx + x] = s1m[t * nx + x]

    pl.semaphore_wait(barrier, len(xpeers) + jnp.where(z == spots[0], nx, jnp.where(z == spots[1], 1, cores)))

    for px, pt in xpeers:
        remote(s1.at[pt * nx + px], r1.at[t * nx + x], s1s_sem, s1r_sem, at(px, z, pt)).start()
        remote(s1m.at[pt * nx + px], r1m.at[t * nx + x], m1s_sem, m1r_sem, at(px, z, pt)).start()

    def bulk(ref, blocks, send, recv):
        part = ref.at[pl.ds(0, blocks)]
        return remote(part, part, send, recv, at(x, z, (t + 1) % cores))

    bulk(r1m, len(xpeers), m1s_sem, m1r_sem).wait_recv()
    bulk(r1, len(xpeers), s1s_sem, s1r_sem).wait_recv()

    def merged(ml):
        top = functools.reduce(jnp.maximum, ml)
        fs = [jnp.exp2((m - top) * scale) for m in ml]
        tot = functools.reduce(jnp.add, [f * pltpu.roll(m, half, 1) for f, m in zip(fs, ml)])
        return top, fs, tot

    for o in reversed(range(cores)):
        top, fs, tot = merged([r1m[o * nx + cx] for cx in range(nx)])
        s2m[o] = jnp.where(lane_s < half, top, pltpu.roll(tot, half, 1))
        for j in range(hq):
            num = functools.reduce(
                jnp.add,
                [jnp.broadcast_to(fs[cx][:, j : j + 1], (sb, hd)) * r1[o * nx + cx, j].astype(F32) for cx in range(nx)])
            s2[o, j] = num.astype(BF16)

        @pl.when(z != spots[o])
        def _():
            remote(s2m.at[o], r2m.at[z], m2s_sem, m2r_sem, at(x, spots[o], t)).start()
            remote(s2.at[o], r2.at[z], s2s_sem, s2r_sem, at(x, spots[o], t)).start()

        @pl.when(z == spots[o])
        def _():
            r2[z] = s2[o]
            r2m[z] = s2m[o]

    w_send = remote(w_v.at[t], w_v.at[t], ws_sem, wr_sem, at(x, z, (t + 1) % cores))
    w_recv = remote(w_v.at[t], w_v.at[(t + 1) % cores], ws_sem, wr_sem, at(x, z, (t + 1) % cores))
    w_copy.wait()
    w_send.start()

    def direct(dx):
        to = at((x + dx) % nx, spots[1], t)
        return remote(g_v.at[x, 0], g_v.at[x, 0], gzs_sem, peer_sem.at[0] if dx else own_sem.at[0], to)

    def along_z(o, pz):
        return remote(g_v.at[x, o], g_v.at[x, o], gzs_sem, own_sem.at[o], at(x, pz, t))

    def along_x(o, dx):
        return remote(g_v.at[x, o], g_v.at[x, o], gxs_sem, peer_sem.at[o], at((x + dx) % nx, z, t))

    def own_arrival(o):
        return remote(g_v.at[x, o], g_v.at[x, o], gzs_sem, own_sem.at[o], at(x, z, (t + 1) % cores))

    xorder = [d for d in range(nx) if d]
    for o in reversed(range(cores)):
        zorder = [(spots[o] + d) % nz for d in range(1, nz)]
        if o == 0:
            zorder = [pz for pz in zorder if pz != spots[1]]

        @pl.when(z == spots[o])
        def _():
            bulk(r2m, nz - 1, m2s_sem, m2r_sem).wait_recv()
            bulk(r2, nz - 1, s2s_sem, s2r_sem).wait_recv()
            top, fs, tot = merged([r2m[i] for i in range(nz)])
            inv = jnp.where(lane_s < hq, 1.0 / tot, 0.0)
            fs = [f * inv for f in fs]
            for j in range(hq):
                att = functools.reduce(
                    jnp.add,
                    [jnp.broadcast_to(fs[i][:, j : j + 1], (sb, hd)) * r2[i, j].astype(F32) for i in range(nz)])
                g_v[x, o, j] = att.astype(BF16)
            if o == 0:
                for dx in xorder + [0]:
                    direct(dx).start()
            else:
                for dx in xorder:
                    along_x(o, dx).start()
            for pz in zorder:
                along_z(o, pz).start()
            if o == 0:
                for dx in xorder:
                    along_x(o, dx).start()

    for o in reversed(range(cores)):
        @pl.when((z != spots[o]) & ((z != spots[1]) | (o == 1)))
        def _():
            own_arrival(o).wait_recv()
            for dx in xorder:
                along_x(o, dx).start()

    @pl.when(z == spots[1])
    def _():
        own_arrival(0).wait_recv()

    w_recv.wait_recv()

    def bytes_of(blocks, send, recv):
        part = k_v.at[pl.ds(0, blocks * hq * sb)]
        return remote(part, part, send, recv, at(x, z, (t + 1) % cores))

    out = jnp.zeros((sb, hd), F32)
    for mine in (True, False):
        for o in reversed(range(cores)):
            if not mine:
                bytes_of(nx - 1, gxs_sem, peer_sem.at[o]).wait_recv()
            for dx in [0] if mine else xorder:
                sx = (x + dx) % nx
                for j in range(0, hq, 2):
                    lhs = jnp.concatenate([g_v[sx, o, j], g_v[sx, o, j + 1]], axis=1)
                    first = pl.multiple_of((sx * hq + j) * hd, 2 * hd)
                    out = out + jnp.dot(lhs, w_v[o, pl.ds(first, 2 * hd), :], preferred_element_type=F32)
    out_ref[...] = out.astype(out_ref.dtype)

    w_send.wait_send()
    bulk(s1, len(xpeers), s1s_sem, s1r_sem).wait_send()
    bulk(s1m, len(xpeers), m1s_sem, m1r_sem).wait_send()

    @pl.when((z != spots[0]) & (z != spots[1]))
    def _():
        bulk(s2, cores, s2s_sem, s2r_sem).wait_send()
        bulk(s2m, cores, m2s_sem, m2r_sem).wait_send()

    @pl.when((z == spots[0]) | (z == spots[1]))
    def _():
        bulk(s2, 1, s2s_sem, s2r_sem).wait_send()
        bulk(s2m, 1, m2s_sem, m2r_sem).wait_send()

    @pl.when(z == spots[0])
    def _():
        bytes_of(nz - 2 + nx, gzs_sem, own_sem.at[0]).wait_send()

    @pl.when(z == spots[1])
    def _():
        bytes_of(nz - 1, gzs_sem, own_sem.at[0]).wait_send()
        bytes_of(nx - 1, gxs_sem, peer_sem.at[1]).wait_send()

    @pl.when(z != spots[1])
    def _():
        bytes_of(cores * (nx - 1), gxs_sem, peer_sem.at[0]).wait_send()


def body(query, key_cache, value_cache, lengths, page_order, out_weight):
    pages, page_len, kvh, hd = key_cache.shape
    ns, hl = query.shape[0], query.shape[1]
    cores = lax.axis_size("tensor")
    nz = ns
    nx = lax.axis_size("seq") // nz
    hq = hl // nx
    sb = ns // cores
    rows = page_len * kvh
    pr = page_order.shape[0] // LANES
    wr, wc = out_weight.shape
    dims = (nx, nz, pages, page_len, kvh, ns, hl, hd, cores)
    steps = pages // PAGES_PER_STEP
    dma = pltpu.SemaphoreType.DMA
    return pl.pallas_call(
        functools.partial(kernel, dims),
        out_shape=pltpu.VMEM((sb, wc), BF16),
        in_specs=[pl.BlockSpec(memory_space=pl.ANY)] * 6,
        out_specs=pl.BlockSpec(memory_space=pltpu.VMEM),
        scratch_shapes=[
            pltpu.SMEM((ns,), I32),
            pltpu.VMEM((ns, hl, hd), BF16),
            pltpu.VMEM((pages * rows, hd), BF16),
            pltpu.VMEM((pages * rows, hd), BF16),
            pltpu.VMEM((pr, LANES), I32),
            pltpu.VMEM((cores, wr, wc), BF16),
            pltpu.VMEM((pr, LANES), F32),
            pltpu.VMEM((8, LANES), I32),
            pltpu.SMEM((8, LANES), I32),
            pltpu.VMEM((hl, rows), I32),
            pltpu.VMEM((pages, hl, rows), BF16),
            pltpu.VMEM((pages, hl, LANES), F32),
            pltpu.VMEM((pages, hl, LANES), F32),
            pltpu.VMEM((pages + 1, hl, LANES), F32),
            pltpu.VMEM((pages + 1, hl, LANES), F32),
            pltpu.VMEM((pages + 1, hl, hd), F32),
            pltpu.VMEM((ns, hl, hd), F32),
            pltpu.VMEM((cores * nx, hq, sb, hd), BF16),
            pltpu.VMEM((cores * nx, hq, sb, hd), BF16),
            pltpu.VMEM((cores, hq, sb, hd), BF16),
            pltpu.VMEM((nz, hq, sb, hd), BF16),
            pltpu.VMEM((cores * nx, sb, LANES), F32),
            pltpu.VMEM((cores * nx, sb, LANES), F32),
            pltpu.VMEM((cores, sb, LANES), F32),
            pltpu.VMEM((nz, sb, LANES), F32),
            pltpu.VMEM((nx, cores, hq, sb, hd), BF16),
            dma, dma, dma((steps,)), dma((steps,)), dma, dma, dma, dma, dma,
            dma, dma, dma, dma, dma, dma, dma, dma, dma, dma, dma((cores,)), dma((cores,)),
        ],
        compiler_params=pltpu.CompilerParams(collective_id=0, has_side_effects=True),
        name="paged_decode",
    )(
        lengths, query, key_cache.reshape(pages * rows, hd), value_cache.reshape(pages * rows, hd),
        page_order.reshape(pr, LANES), out_weight)


def solution(mesh):
    in_specs = (
        P("group", "tensor", None),
        P(("group", "seq"), None, "tensor", None),
        P(("group", "seq"), None, "tensor", None),
        P("group"),
        P("group"),
        P("tensor", "seq"),
    )
    out_specs = P(("group", "tensor"), "seq")
    return jax.shard_map(body, mesh=mesh, in_specs=in_specs, out_specs=out_specs, check_vma=False)
```

```python
import functools
import math

import jax
import jax.numpy as jnp
from jax import lax
from jax.experimental import pallas as pl
from jax.experimental.pallas import tpu as pltpu
from jax.sharding import PartitionSpec as P

MESH = pl.DeviceIdType.MESH
F32 = jnp.float32
BF16 = jnp.bfloat16
I32 = jnp.int32
LANES = 128
NEG = -1e30
PAGES_PER_STEP = 8


def kernel(
    dims,
    len_hbm, q_hbm, k_hbm, v_hbm, po_hbm, w_hbm, out_ref,
    len_s, q_v, k_v, v_v, po_v, w_v, val_v, meta_v, meta_s, cmod_v,
    wt_v, mtop, ltot, mrun, lrun, orun, ofin, s1, r1, s2, r2, s2m, r2m, g_v,
    len_sem, q_sem, k_sem, v_sem, po_sem, w_sem, meta_sem, ws_sem, wr_sem,
    s1s_sem, s1r_sem, s2s_sem, s2r_sem, m2s_sem, m2r_sem, gzs_sem, gxs_sem, own_sem, peer_sem,
):
    nx, nz, pages, page_len, kvh, ns, hl, hd, cores = dims
    rows = page_len * kvh
    hq = hl // nx
    sb = ns // cores
    group_size = hl // kvh
    scale = math.log2(math.e) / math.sqrt(hd)
    me = lax.axis_index("seq")
    t = lax.axis_index("tensor")
    x = me // nz
    z = me % nz
    steps = pages // PAGES_PER_STEP
    spots = (1, 0)
    zp = z % 2
    hh = hq // 2

    def at(px, pz, pt):
        return {"seq": px * nz + pz, "tensor": pt}

    def remote(src, dst, send, recv, to):
        return pltpu.make_async_remote_copy(
            src_ref=src, dst_ref=dst, send_sem=send, recv_sem=recv, device_id=to, device_id_type=MESH)

    len_copy = pltpu.make_async_copy(len_hbm, len_s, len_sem)
    len_copy.start()
    po_copy = pltpu.make_async_copy(po_hbm, po_v, po_sem)
    po_copy.start()
    q_copy = pltpu.make_async_copy(q_hbm, q_v, q_sem)
    q_copy.start()

    peers = []
    for dx in [nx // 2] + [d for d in range(nx) if d != nx // 2]:
        for dp in range(2):
            for dt in range(cores):
                if dx or dp or dt:
                    peers.append(((x + dx) % nx, (zp + dp) % 2, (t + dt) % cores))
    barrier = pltpu.get_barrier_semaphore()

    def greet(px, pz, pt):
        pl.semaphore_signal(barrier, inc=1, device_id=at(px, pz, pt), device_id_type=MESH)

    early_greets = 4
    for px, pp, pt in peers[:early_greets]:
        greet(px, z - zp + pp, pt)

    step_rows = PAGES_PER_STEP * rows

    def kv_copy(src, dst, sem, c):
        part = pl.ds(c * step_rows, step_rows)
        return pltpu.make_async_copy(src.at[part], dst.at[part], sem.at[c])

    for c in range(steps):
        kv_copy(k_hbm, k_v, k_sem, c).start()
    for c in range(steps):
        kv_copy(v_hbm, v_v, v_sem, c).start()
    w_copy = pltpu.make_async_copy(w_hbm, w_v.at[t], w_sem)
    w_copy.start()

    for px, pp, pt in peers[early_greets:]:
        greet(px, z - zp + pp, pt)

    @pl.when(z < 2)
    def _():
        for d in range(2, nz, 2):
            greet(x, z + d, t)

    cl = lax.broadcasted_iota(I32, (hl, rows), 1)
    hr = lax.broadcasted_iota(I32, (hl, rows), 0)
    cmod_v[...] = jnp.where(cl % kvh == hr // group_size, cl, 1 << 20)
    mrun[0] = jnp.full((hl, LANES), NEG, F32)
    lrun[0] = jnp.zeros((hl, LANES), F32)
    orun[0] = jnp.zeros((hl, hd), F32)

    len_copy.wait()
    lens = [len_s[s] for s in range(ns)]
    starts = []
    run = jnp.int32(0)
    for s in range(ns):
        starts.append(run)
        run = run + lax.shift_right_logical(lens[s] + (page_len - 1), int(math.log2(page_len)))
    pr = po_v.shape[0]
    rank = lax.broadcasted_iota(I32, (pr, LANES), 0) * LANES + lax.broadcasted_iota(I32, (pr, LANES), 1)
    owner = jnp.zeros((pr, LANES), I32)
    end = jnp.full((pr, LANES), lens[0], I32)
    for s in range(1, ns):
        past = rank >= starts[s]
        owner = jnp.where(past, s, owner)
        end = jnp.where(past, lens[s] + starts[s] * page_len, end)
    valid = jnp.clip(end - rank * page_len, 0, page_len)
    owner = jnp.where(valid > 0, owner, ns)
    val_v[...] = (owner * 256 + valid).astype(F32)

    po_copy.wait()
    ids = lax.broadcasted_iota(I32, (pages, LANES), 0) + me * pages
    acc = jnp.zeros((pages, LANES), F32)
    for i in range(pr):
        hit = jnp.broadcast_to(po_v[i : i + 1, :], (pages, LANES)) == ids
        acc = acc + jnp.where(hit, jnp.broadcast_to(val_v[i : i + 1, :], (pages, LANES)), 0.0)
    val_col = jnp.broadcast_to(jnp.sum(acc, axis=1, keepdims=True), (pages, LANES))
    pad = jnp.concatenate([val_col, jnp.zeros((LANES - pages, LANES), F32)], axis=0)
    val_row = jnp.transpose(pad)[0:1, :]
    own_col = lax.shift_right_logical(val_col.astype(I32), 8)
    val_row_i = val_row.astype(I32)
    own_row = lax.shift_right_logical(val_row_i, 8)
    prow = lax.broadcasted_iota(I32, (pages, LANES), 0)
    lane = lax.broadcasted_iota(I32, (pages, LANES), 1)
    same = (own_col == jnp.broadcast_to(own_row, (pages, LANES))) & (prow < lane)
    prev = jnp.max(jnp.where(same, (prow + 1).astype(F32), 0.0), axis=0, keepdims=True).astype(I32)
    last = jnp.max(jnp.where(own_col == lane, (prow + 1).astype(F32), 0.0), axis=0, keepdims=True).astype(I32)
    meta_v[0:1, :] = prev * 8192 + val_row_i
    meta_v[1:2, :] = last
    meta_copy = pltpu.make_async_copy(meta_v, meta_s, meta_sem)
    meta_copy.start()
    meta_copy.wait()
    q_copy.wait()

    def page_part(p):
        return pl.ds(pl.multiple_of(p * rows, rows), rows)

    def score_step(c, carry):
        kv_copy(k_hbm, k_v, k_sem, c).wait()
        for i in range(PAGES_PER_STEP):
            p = c * PAGES_PER_STEP + i
            code = meta_s[0, p]
            nvalid = jnp.bitwise_and(code, 255) * kvh
            own = jnp.minimum(jnp.bitwise_and(lax.shift_right_logical(code, 8), 31), ns - 1)
            before = jnp.clip(lax.shift_right_logical(code, 13), 0, pages)
            sc = lax.dot_general(
                q_v[own], k_v[page_part(p), :], (((1,), (1,)), ((), ())), preferred_element_type=F32)
            sc = jnp.where(cmod_v[...] < nvalid, sc, NEG)
            top = jnp.max(sc, axis=1, keepdims=True)
            wt = jnp.exp2((sc - top) * scale)
            wt_v[p] = wt.astype(BF16)
            top = jnp.broadcast_to(top, (hl, LANES))
            mtop[p] = top
            ltot[p] = jnp.broadcast_to(jnp.sum(wt, axis=1, keepdims=True), (hl, LANES))
            mrun[p + 1] = jnp.maximum(mrun[before], top)
        return carry

    lax.fori_loop(0, steps, score_step, 0)

    def value_step(c, carry):
        kv_copy(v_hbm, v_v, v_sem, c).wait()
        for i in range(PAGES_PER_STEP):
            p = c * PAGES_PER_STEP + i
            code = meta_s[0, p]
            own = jnp.bitwise_and(lax.shift_right_logical(code, 8), 31)
            before = jnp.clip(lax.shift_right_logical(code, 13), 0, pages)
            final = jnp.clip(meta_s[1, own], 0, pages)
            o = jnp.dot(wt_v[p], v_v[page_part(p), :], preferred_element_type=F32)
            fb = jnp.exp2((mtop[p] - mrun[final]) * scale)
            lrun[p + 1] = lrun[before] + fb * ltot[p]
            orun[p + 1] = orun[before] + fb * o
        return carry

    lax.fori_loop(0, steps, value_step, 0)

    lane_h = lax.broadcasted_iota(I32, (hl, LANES), 1)
    half = LANES // 2
    ml = jnp.zeros((hl, LANES), F32)
    for s in range(ns):
        f = jnp.clip(meta_s[1, s], 0, pages)
        ofin[s] = orun[f]
        ml = jnp.where(lane_h == s, mrun[f], ml)
        ml = jnp.where(lane_h == half + s, lrun[f], ml)
    ml_a = ml.astype(BF16).astype(F32)
    ml_b = (ml - ml_a).astype(BF16).astype(F32)
    ml_c = ml - ml_a - ml_b
    none = jnp.zeros((hh, LANES), F32)
    for cx in range(nx):
        for cp in range(2):
            h0 = cx * hq + cp * hh
            tail = jnp.concatenate(
                [ml_a[h0 : h0 + hh], ml_b[h0 : h0 + hh], ml_c[h0 : h0 + hh], none], axis=0).astype(BF16)
            for ct in range(cores):
                d = (cx * 2 + cp) * cores + ct
                s1[d, hh] = tail[: 2 * hh]
                s1[d, hh + 1] = tail[2 * hh :]
                for j in range(hh):
                    s1[d, j] = ofin[ct * sb : (ct + 1) * sb, h0 + j, :].astype(BF16)
    here = (t * nx + x) * 2 + zp
    r1[here] = s1[(x * 2 + zp) * cores + t]

    pl.semaphore_wait(barrier, len(peers) + jnp.where(z < 2, 0, 1))

    for px, pp, pt in peers:
        remote(s1.at[(px * 2 + pp) * cores + pt], r1.at[here], s1s_sem, s1r_sem, at(px, z - zp + pp, pt)).start()

    def bulk(ref, blocks, send, recv):
        part = ref.at[pl.ds(0, blocks)]
        return remote(part, part, send, recv, at(x, z, (t + 1) % cores))

    bulk(r1, len(peers), s1s_sem, s1r_sem).wait_recv()

    hn = cores * hh
    row_h = lax.broadcasted_iota(I32, (hn, LANES), 0)
    lane_r = lax.broadcasted_iota(I32, (hn, LANES), 1)

    def merged(ml):
        top = functools.reduce(jnp.maximum, ml)
        fs = [jnp.exp2((m - top) * scale) for m in ml]
        tot = functools.reduce(jnp.add, [f * pltpu.roll(m, half, 1) for f, m in zip(fs, ml)])
        return top, fs, tot

    def as_columns(fs):
        pad = jnp.zeros((LANES - len(fs) * hn, LANES), F32)
        ft = jnp.transpose(jnp.concatenate(fs + [pad], axis=0))
        return jnp.where(t == 0, ft[:sb], ft[sb : 2 * sb])

    def source_ml(i):
        both = []
        for ct in range(cores):
            k = ct * nx * 2 + i
            y = r1[k, hh].astype(F32) + r1[k, hh + 1].astype(F32)
            both.append(y + pltpu.roll(y, hh, 0))
        return jnp.where(row_h < hh, both[0], both[1])

    top, fs, tot = merged([source_ml(i) for i in range(nx * 2)])
    s2m[...] = jnp.where(lane_r < half, top, pltpu.roll(tot, half, 1))
    ft = as_columns(fs)
    for ct in range(cores):
        for j in range(hh):
            k = ct * hh + j
            num = functools.reduce(
                jnp.add,
                [jnp.broadcast_to(ft[:, i * hn + k : i * hn + k + 1], (sb, hd)) * r1[ct * nx * 2 + i, j].astype(F32)
                 for i in range(nx * 2)])
            s2[k] = num.astype(BF16)

    @pl.when(z >= 2)
    def _():
        remote(s2m, r2m.at[z // 2], m2s_sem, m2r_sem, at(x, zp, t)).start()
        remote(s2, r2.at[z // 2], s2s_sem, s2r_sem, at(x, zp, t)).start()

    @pl.when(z < 2)
    def _():
        r2[0] = s2[...]
        r2m[0] = s2m[...]

    w_send = remote(w_v.at[t], w_v.at[t], ws_sem, wr_sem, at(x, z, (t + 1) % cores))
    w_recv = remote(w_v.at[t], w_v.at[(t + 1) % cores], ws_sem, wr_sem, at(x, z, (t + 1) % cores))
    w_copy.wait()
    w_send.start()

    def direct(dx):
        to = at((x + dx) % nx, spots[1], t)
        return remote(g_v.at[x, 0], g_v.at[x, 0], gzs_sem, peer_sem.at[0] if dx else own_sem.at[0], to)

    def along_z(o, pz):
        return remote(g_v.at[x, o], g_v.at[x, o], gzs_sem, own_sem.at[o], at(x, pz, t))

    def along_x(o, dx):
        return remote(g_v.at[x, o], g_v.at[x, o], gxs_sem, peer_sem.at[o], at((x + dx) % nx, z, t))

    def own_arrival(o):
        return remote(g_v.at[x, o], g_v.at[x, o], gzs_sem, own_sem.at[o], at(x, z, (t + 1) % cores))

    xorder = [d for d in range(nx) if d]
    for o in reversed(range(cores)):
        zorder = [(spots[o] + d) % nz for d in range(1, nz)]
        if o == 0:
            zorder = [pz for pz in zorder if pz != spots[1]]

        @pl.when(z == spots[o])
        def _():
            bulk(r2m, nz // 2 - 1, m2s_sem, m2r_sem).wait_recv()
            bulk(r2, nz // 2 - 1, s2s_sem, s2r_sem).wait_recv()
            top, fs, tot = merged([r2m[i] for i in range(nz // 2)])
            inv = jnp.where(lane_r < ns, 1.0 / tot, 0.0)
            ft = as_columns([f * inv for f in fs])
            for k in range(hn):
                att = functools.reduce(
                    jnp.add,
                    [jnp.broadcast_to(ft[:, i * hn + k : i * hn + k + 1], (sb, hd)) * r2[i, k].astype(F32)
                     for i in range(nz // 2)])
                g_v[x, o, k] = att.astype(BF16)
            if o == 0:
                for dx in xorder + [0]:
                    direct(dx).start()
            else:
                for dx in xorder:
                    along_x(o, dx).start()
            for pz in zorder:
                along_z(o, pz).start()
            if o == 0:
                for dx in xorder:
                    along_x(o, dx).start()

    for o in reversed(range(cores)):
        @pl.when((z != spots[o]) & ((z != spots[1]) | (o == 1)))
        def _():
            own_arrival(o).wait_recv()
            for dx in xorder:
                along_x(o, dx).start()

    @pl.when(z == spots[1])
    def _():
        own_arrival(0).wait_recv()

    w_recv.wait_recv()

    def bytes_of(blocks, send, recv):
        part = k_v.at[pl.ds(0, blocks * hn * sb)]
        return remote(part, part, send, recv, at(x, z, (t + 1) % cores))

    out = jnp.zeros((sb, hd), F32)
    for mine in (True, False):
        for o in reversed(range(cores)):
            if not mine:
                bytes_of(nx - 1, gxs_sem, peer_sem.at[o]).wait_recv()
            for dx in [0] if mine else xorder:
                sx = (x + dx) % nx
                for k in range(0, hn, 2):
                    lhs = jnp.concatenate([g_v[sx, o, k], g_v[sx, o, k + 1]], axis=1)
                    head = sx * hq + (1 - o) * hh + k % hh
                    first = pl.multiple_of(head * hd, 2 * hd)
                    out = out + jnp.dot(lhs, w_v[k // hh, pl.ds(first, 2 * hd), :], preferred_element_type=F32)
    out_ref[...] = out.astype(out_ref.dtype)

    w_send.wait_send()
    bulk(s1, len(peers), s1s_sem, s1r_sem).wait_send()

    @pl.when(z >= 2)
    def _():
        remote(s2, s2, s2s_sem, s2r_sem, at(x, z, (t + 1) % cores)).wait_send()
        remote(s2m, s2m, m2s_sem, m2r_sem, at(x, z, (t + 1) % cores)).wait_send()

    @pl.when(z == spots[0])
    def _():
        bytes_of(nz - 2 + nx, gzs_sem, own_sem.at[0]).wait_send()

    @pl.when(z == spots[1])
    def _():
        bytes_of(nz - 1, gzs_sem, own_sem.at[0]).wait_send()
        bytes_of(nx - 1, gxs_sem, peer_sem.at[1]).wait_send()

    @pl.when(z != spots[1])
    def _():
        bytes_of(cores * (nx - 1), gxs_sem, peer_sem.at[0]).wait_send()


def body(query, key_cache, value_cache, lengths, page_order, out_weight):
    pages, page_len, kvh, hd = key_cache.shape
    ns, hl = query.shape[0], query.shape[1]
    cores = lax.axis_size("tensor")
    nz = ns
    nx = lax.axis_size("seq") // nz
    hh = hl // nx // 2
    sb = ns // cores
    rows = page_len * kvh
    pr = page_order.shape[0] // LANES
    wr, wc = out_weight.shape
    dims = (nx, nz, pages, page_len, kvh, ns, hl, hd, cores)
    steps = pages // PAGES_PER_STEP
    dma = pltpu.SemaphoreType.DMA
    return pl.pallas_call(
        functools.partial(kernel, dims),
        out_shape=pltpu.VMEM((sb, wc), BF16),
        in_specs=[pl.BlockSpec(memory_space=pl.ANY)] * 6,
        out_specs=pl.BlockSpec(memory_space=pltpu.VMEM),
        scratch_shapes=[
            pltpu.SMEM((ns,), I32),
            pltpu.VMEM((ns, hl, hd), BF16),
            pltpu.VMEM((pages * rows, hd), BF16),
            pltpu.VMEM((pages * rows, hd), BF16),
            pltpu.VMEM((pr, LANES), I32),
            pltpu.VMEM((cores, wr, wc), BF16),
            pltpu.VMEM((pr, LANES), F32),
            pltpu.VMEM((8, LANES), I32),
            pltpu.SMEM((8, LANES), I32),
            pltpu.VMEM((hl, rows), I32),
            pltpu.VMEM((pages, hl, rows), BF16),
            pltpu.VMEM((pages, hl, LANES), F32),
            pltpu.VMEM((pages, hl, LANES), F32),
            pltpu.VMEM((pages + 1, hl, LANES), F32),
            pltpu.VMEM((pages + 1, hl, LANES), F32),
            pltpu.VMEM((pages + 1, hl, hd), F32),
            pltpu.VMEM((ns, hl, hd), F32),
            pltpu.VMEM((cores * nx * 2, hh + 2, sb, hd), BF16),
            pltpu.VMEM((cores * nx * 2, hh + 2, sb, hd), BF16),
            pltpu.VMEM((cores * hh, sb, hd), BF16),
            pltpu.VMEM((nz // 2, cores * hh, sb, hd), BF16),
            pltpu.VMEM((cores * hh, LANES), F32),
            pltpu.VMEM((nz // 2, cores * hh, LANES), F32),
            pltpu.VMEM((nx, 2, cores * hh, sb, hd), BF16),
            dma, dma, dma((steps,)), dma((steps,)), dma, dma, dma, dma, dma,
            dma, dma, dma, dma, dma, dma, dma, dma, dma((2,)), dma((2,)),
        ],
        compiler_params=pltpu.CompilerParams(collective_id=0, has_side_effects=True),
        name="paged_decode",
    )(
        lengths, query, key_cache.reshape(pages * rows, hd), value_cache.reshape(pages * rows, hd),
        page_order.reshape(pr, LANES), out_weight)


def solution(mesh):
    in_specs = (
        P("group", "tensor", None),
        P(("group", "seq"), None, "tensor", None),
        P(("group", "seq"), None, "tensor", None),
        P("group"),
        P("group"),
        P("tensor", "seq"),
    )
    out_specs = P(("group", "tensor"), "seq")
    return jax.shard_map(body, mesh=mesh, in_specs=in_specs, out_specs=out_specs, check_vma=False)
```

```python
import functools
import math

import jax
import jax.numpy as jnp
from jax import lax
from jax.experimental import pallas as pl
from jax.experimental.pallas import tpu as pltpu
from jax.sharding import PartitionSpec as P

MESH = pl.DeviceIdType.MESH
F32 = jnp.float32
BF16 = jnp.bfloat16
I32 = jnp.int32
LANES = 128
NEG = -1e30
K_PARTS = (12, 20)
V_PARTS = (32,)


def kernel(
    dims,
    len_hbm, q_hbm, k_hbm, v_hbm, po_hbm, w_hbm, out_ref,
    len_s, q_v, k_v, v_v, po_v, w_v, val_v, meta_v, meta_s, cmod_v,
    wt_v, mtop, ltot, mrun, lrun, orun, ofin, s1, r1, s2, r2, g_v,
    len_sem, q_sem, k_sem, v_sem, po_sem, w_sem, meta_sem, ws_sem, wr_sem,
    s1s_sem, s1r_sem, s2s_sem, s2r_sem, gzs_sem, gxs_sem, own_sem, peer_sem,
):
    nx, nz, pages, page_len, kvh, ns, hl, hd, cores = dims
    rows = page_len * kvh
    hq = hl // nx
    sb = ns // cores
    group_size = hl // kvh
    scale = math.log2(math.e) / math.sqrt(hd)
    me = lax.axis_index("seq")
    t = lax.axis_index("tensor")
    x = me // nz
    z = me % nz
    spots = (1, 0)
    zp = z % 2
    hh = hq // 2

    def at(px, pz, pt):
        return {"seq": px * nz + pz, "tensor": pt}

    def remote(src, dst, send, recv, to):
        return pltpu.make_async_remote_copy(
            src_ref=src, dst_ref=dst, send_sem=send, recv_sem=recv, device_id=to, device_id_type=MESH)

    len_copy = pltpu.make_async_copy(len_hbm, len_s, len_sem)
    len_copy.start()
    po_copy = pltpu.make_async_copy(po_hbm, po_v, po_sem)
    po_copy.start()
    q_copy = pltpu.make_async_copy(q_hbm, q_v, q_sem)
    q_copy.start()

    peers = []
    for dx in [nx // 2] + [d for d in range(nx) if d != nx // 2]:
        for dp in range(2):
            for dt in range(cores):
                if dx or dp or dt:
                    peers.append(((x + dx) % nx, (zp + dp) % 2, (t + dt) % cores))
    barrier = pltpu.get_barrier_semaphore()

    def greet(px, pz, pt):
        pl.semaphore_signal(barrier, inc=1, device_id=at(px, pz, pt), device_id_type=MESH)

    early_greets = 4
    for px, pp, pt in peers[:early_greets]:
        greet(px, z - zp + pp, pt)

    def kv_copies(src, dst, sem, shares):
        copies, first = [], 0
        for i, share in enumerate(shares):
            count = pages * share // sum(shares)
            part = pl.ds(first * rows, count * rows)
            copies.append((pltpu.make_async_copy(src.at[part], dst.at[part], sem.at[i]), range(first, first + count)))
            first += count
        return copies

    k_copies = kv_copies(k_hbm, k_v, k_sem, K_PARTS)
    v_copies = kv_copies(v_hbm, v_v, v_sem, V_PARTS)
    for copy, _ in k_copies + v_copies:
        copy.start()
    w_copy = pltpu.make_async_copy(w_hbm, w_v.at[t], w_sem)
    w_copy.start()

    for px, pp, pt in peers[early_greets:]:
        greet(px, z - zp + pp, pt)

    @pl.when(z < 2)
    def _():
        for d in range(2, nz, 2):
            greet(x, z + d, t)

    cl = lax.broadcasted_iota(I32, (hl, rows), 1)
    hr = lax.broadcasted_iota(I32, (hl, rows), 0)
    cmod_v[...] = jnp.where(cl % kvh == hr // group_size, cl, 1 << 20)
    mrun[0] = jnp.full((hl, LANES), NEG, F32)
    lrun[0] = jnp.zeros((hl, LANES), F32)
    orun[0] = jnp.zeros((hl, hd), F32)

    len_copy.wait()
    lens = [len_s[s] for s in range(ns)]
    starts = []
    run = jnp.int32(0)
    for s in range(ns):
        starts.append(run)
        run = run + lax.shift_right_logical(lens[s] + (page_len - 1), int(math.log2(page_len)))
    pr = po_v.shape[0]
    rank = lax.broadcasted_iota(I32, (pr, LANES), 0) * LANES + lax.broadcasted_iota(I32, (pr, LANES), 1)
    owner = jnp.zeros((pr, LANES), I32)
    end = jnp.full((pr, LANES), lens[0], I32)
    for s in range(1, ns):
        past = rank >= starts[s]
        owner = jnp.where(past, s, owner)
        end = jnp.where(past, lens[s] + starts[s] * page_len, end)
    valid = jnp.clip(end - rank * page_len, 0, page_len)
    owner = jnp.where(valid > 0, owner, ns)
    val_v[...] = (owner * 256 + valid).astype(F32)

    po_copy.wait()
    ids = lax.broadcasted_iota(I32, (pages, LANES), 0) + me * pages
    acc = jnp.zeros((pages, LANES), F32)
    for i in range(pr):
        hit = jnp.broadcast_to(po_v[i : i + 1, :], (pages, LANES)) == ids
        acc = acc + jnp.where(hit, jnp.broadcast_to(val_v[i : i + 1, :], (pages, LANES)), 0.0)
    val_col = jnp.broadcast_to(jnp.sum(acc, axis=1, keepdims=True), (pages, LANES))
    pad = jnp.concatenate([val_col, jnp.zeros((LANES - pages, LANES), F32)], axis=0)
    val_row = jnp.transpose(pad)[0:1, :]
    own_col = lax.shift_right_logical(val_col.astype(I32), 8)
    val_row_i = val_row.astype(I32)
    own_row = lax.shift_right_logical(val_row_i, 8)
    prow = lax.broadcasted_iota(I32, (pages, LANES), 0)
    lane = lax.broadcasted_iota(I32, (pages, LANES), 1)
    same = (own_col == jnp.broadcast_to(own_row, (pages, LANES))) & (prow < lane)
    prev = jnp.max(jnp.where(same, (prow + 1).astype(F32), 0.0), axis=0, keepdims=True).astype(I32)
    last = jnp.max(jnp.where(own_col == lane, (prow + 1).astype(F32), 0.0), axis=0, keepdims=True).astype(I32)
    meta_v[0:1, :] = prev * 8192 + val_row_i
    meta_v[1:2, :] = last
    meta_copy = pltpu.make_async_copy(meta_v, meta_s, meta_sem)
    meta_copy.start()
    meta_copy.wait()
    q_copy.wait()

    def page_part(p):
        return pl.ds(p * rows, rows)

    for copy, part in k_copies:
        copy.wait()
        for p in part:
            code = meta_s[0, p]
            nvalid = jnp.bitwise_and(code, 255) * kvh
            own = jnp.minimum(jnp.bitwise_and(lax.shift_right_logical(code, 8), 31), ns - 1)
            before = jnp.clip(lax.shift_right_logical(code, 13), 0, pages)
            sc = lax.dot_general(
                q_v[own], k_v[page_part(p), :], (((1,), (1,)), ((), ())), preferred_element_type=F32)
            sc = jnp.where(cmod_v[...] < nvalid, sc, NEG)
            top = jnp.max(sc, axis=1, keepdims=True)
            wt = jnp.exp2((sc - top) * scale)
            wt_v[p] = wt.astype(BF16)
            top = jnp.broadcast_to(top, (hl, LANES))
            mtop[p] = top
            ltot[p] = jnp.broadcast_to(jnp.sum(wt, axis=1, keepdims=True), (hl, LANES))
            mrun[p + 1] = jnp.maximum(mrun[before], top)

    for copy, part in v_copies:
        copy.wait()
        for p in part:
            code = meta_s[0, p]
            own = jnp.bitwise_and(lax.shift_right_logical(code, 8), 31)
            before = jnp.clip(lax.shift_right_logical(code, 13), 0, pages)
            final = jnp.clip(meta_s[1, own], 0, pages)
            o = jnp.dot(wt_v[p], v_v[page_part(p), :], preferred_element_type=F32)
            fb = jnp.exp2((mtop[p] - mrun[final]) * scale)
            lrun[p + 1] = lrun[before] + fb * ltot[p]
            orun[p + 1] = orun[before] + fb * o

    lane_h = lax.broadcasted_iota(I32, (hl, LANES), 1)
    half = LANES // 2
    ml = jnp.zeros((hl, LANES), F32)
    for s in range(ns):
        f = jnp.clip(meta_s[1, s], 0, pages)
        ofin[s] = orun[f]
        ml = jnp.where(lane_h == s, mrun[f], ml)
        ml = jnp.where(lane_h == half + s, lrun[f], ml)
    hn = cores * hh
    row_h = lax.broadcasted_iota(I32, (hn, LANES), 0)
    lane_r = lax.broadcasted_iota(I32, (hn, LANES), 1)

    def split(v):
        a = v.astype(BF16).astype(F32)
        b = (v - a).astype(BF16).astype(F32)
        return a + pltpu.roll(b, ns, 1) + pltpu.roll(v - a - b, 2 * ns, 1)

    def joined(v):
        return v + pltpu.roll(v, LANES - ns, 1) + pltpu.roll(v, LANES - 2 * ns, 1)

    ml = split(ml)
    for cx in range(nx):
        for cp in range(2):
            h0 = cx * hq + cp * hh
            tail = jnp.concatenate([ml[h0 : h0 + hh]] * cores, axis=0)
            tail = jnp.where(row_h // hh == t, tail, 0.0).astype(BF16)
            for ct in range(cores):
                d = (cx * 2 + cp) * cores + ct
                s1[d, hh] = tail
                for j in range(hh):
                    s1[d, j] = ofin[ct * sb : (ct + 1) * sb, h0 + j, :].astype(BF16)
    here = (t * nx + x) * 2 + zp
    r1[here] = s1[(x * 2 + zp) * cores + t]

    pl.semaphore_wait(barrier, len(peers) + jnp.where(z < 2, 0, 1))

    for px, pp, pt in peers:
        remote(s1.at[(px * 2 + pp) * cores + pt], r1.at[here], s1s_sem, s1r_sem, at(px, z - zp + pp, pt)).start()

    def bulk(ref, blocks, send, recv):
        part = ref.at[pl.ds(0, blocks)]
        return remote(part, part, send, recv, at(x, z, (t + 1) % cores))

    bulk(r1, len(peers), s1s_sem, s1r_sem).wait_recv()

    def merged(ml):
        top = functools.reduce(jnp.maximum, ml)
        fs = [jnp.exp2((m - top) * scale) for m in ml]
        tot = functools.reduce(jnp.add, [f * pltpu.roll(m, half, 1) for f, m in zip(fs, ml)])
        return top, fs, tot

    def as_columns(fs):
        pad = jnp.zeros((LANES - len(fs) * hn, LANES), F32)
        ft = jnp.transpose(jnp.concatenate(fs + [pad], axis=0))
        return jnp.where(t == 0, ft[:sb], ft[sb : 2 * sb])

    def source_ml(i):
        return joined(r1[i, hh].astype(F32) + r1[nx * 2 + i, hh].astype(F32))

    top, fs, tot = merged([source_ml(i) for i in range(nx * 2)])
    out_ml = jnp.where(lane_r < half, top, pltpu.roll(tot, half, 1))
    s2[hn] = split(jnp.where(lane_r % half < ns, out_ml, 0.0)).astype(BF16)
    ft = as_columns(fs)
    for ct in range(cores):
        for j in range(hh):
            k = ct * hh + j
            num = functools.reduce(
                jnp.add,
                [jnp.broadcast_to(ft[:, i * hn + k : i * hn + k + 1], (sb, hd)) * r1[ct * nx * 2 + i, j].astype(F32)
                 for i in range(nx * 2)])
            s2[k] = num.astype(BF16)

    @pl.when(z >= 2)
    def _():
        remote(s2, r2.at[z // 2], s2s_sem, s2r_sem, at(x, zp, t)).start()

    @pl.when(z < 2)
    def _():
        r2[0] = s2[...]

    w_send = remote(w_v.at[t], w_v.at[t], ws_sem, wr_sem, at(x, z, (t + 1) % cores))
    w_recv = remote(w_v.at[t], w_v.at[(t + 1) % cores], ws_sem, wr_sem, at(x, z, (t + 1) % cores))
    w_copy.wait()
    w_send.start()

    def direct(dx):
        to = at((x + dx) % nx, spots[1], t)
        return remote(g_v.at[x, 0], g_v.at[x, 0], gzs_sem, peer_sem.at[0] if dx else own_sem.at[0], to)

    def along_z(o, pz):
        return remote(g_v.at[x, o], g_v.at[x, o], gzs_sem, own_sem.at[o], at(x, pz, t))

    def along_x(o, dx):
        return remote(g_v.at[x, o], g_v.at[x, o], gxs_sem, peer_sem.at[o], at((x + dx) % nx, z, t))

    def own_arrival(o):
        return remote(g_v.at[x, o], g_v.at[x, o], gzs_sem, own_sem.at[o], at(x, z, (t + 1) % cores))

    xorder = [d for d in range(nx) if d]
    for o in reversed(range(cores)):
        zorder = [(spots[o] + d) % nz for d in range(1, nz)]
        if o == 0:
            zorder = [pz for pz in zorder if pz != spots[1]]

        @pl.when(z == spots[o])
        def _():
            bulk(r2, nz // 2 - 1, s2s_sem, s2r_sem).wait_recv()
            top, fs, tot = merged([joined(r2[i, hn].astype(F32)) for i in range(nz // 2)])
            inv = jnp.where(lane_r < ns, 1.0 / tot, 0.0)
            ft = as_columns([f * inv for f in fs])
            for k in range(hn):
                att = functools.reduce(
                    jnp.add,
                    [jnp.broadcast_to(ft[:, i * hn + k : i * hn + k + 1], (sb, hd)) * r2[i, k].astype(F32)
                     for i in range(nz // 2)])
                g_v[x, o, k] = att.astype(BF16)
            if o == 0:
                along_z(o, zorder[0]).start()
                for dx in xorder + [0]:
                    direct(dx).start()
            else:
                for dx in xorder:
                    along_x(o, dx).start()
            for pz in zorder[1 if o == 0 else 0 :]:
                along_z(o, pz).start()
            if o == 0:
                for dx in xorder:
                    along_x(o, dx).start()

    for o in reversed(range(cores)):
        @pl.when((z != spots[o]) & ((z != spots[1]) | (o == 1)))
        def _():
            own_arrival(o).wait_recv()
            for dx in xorder:
                along_x(o, dx).start()

    @pl.when(z == spots[1])
    def _():
        own_arrival(0).wait_recv()

    w_recv.wait_recv()

    def bytes_of(blocks, send, recv):
        part = k_v.at[pl.ds(0, blocks * hn * sb)]
        return remote(part, part, send, recv, at(x, z, (t + 1) % cores))

    out = jnp.zeros((sb, hd), F32)
    for mine in (True, False):
        for o in reversed(range(cores)):
            if not mine:
                bytes_of(nx - 1, gxs_sem, peer_sem.at[o]).wait_recv()
            for dx in [0] if mine else xorder:
                sx = (x + dx) % nx
                for k in range(0, hn, 2):
                    lhs = jnp.concatenate([g_v[sx, o, k], g_v[sx, o, k + 1]], axis=1)
                    head = sx * hq + (1 - o) * hh + k % hh
                    first = pl.multiple_of(head * hd, 2 * hd)
                    out = out + jnp.dot(lhs, w_v[k // hh, pl.ds(first, 2 * hd), :], preferred_element_type=F32)
    out_ref[...] = out.astype(out_ref.dtype)

    w_send.wait_send()
    bulk(s1, len(peers), s1s_sem, s1r_sem).wait_send()

    @pl.when(z >= 2)
    def _():
        remote(s2, s2, s2s_sem, s2r_sem, at(x, z, (t + 1) % cores)).wait_send()

    @pl.when(z == spots[0])
    def _():
        bytes_of(nz - 2 + nx, gzs_sem, own_sem.at[0]).wait_send()

    @pl.when(z == spots[1])
    def _():
        bytes_of(nz - 1, gzs_sem, own_sem.at[0]).wait_send()
        bytes_of(nx - 1, gxs_sem, peer_sem.at[1]).wait_send()

    @pl.when(z != spots[1])
    def _():
        bytes_of(cores * (nx - 1), gxs_sem, peer_sem.at[0]).wait_send()


def body(query, key_cache, value_cache, lengths, page_order, out_weight):
    pages, page_len, kvh, hd = key_cache.shape
    ns, hl = query.shape[0], query.shape[1]
    cores = lax.axis_size("tensor")
    nz = ns
    nx = lax.axis_size("seq") // nz
    hh = hl // nx // 2
    sb = ns // cores
    rows = page_len * kvh
    pr = page_order.shape[0] // LANES
    wr, wc = out_weight.shape
    dims = (nx, nz, pages, page_len, kvh, ns, hl, hd, cores)
    dma = pltpu.SemaphoreType.DMA
    return pl.pallas_call(
        functools.partial(kernel, dims),
        out_shape=pltpu.VMEM((sb, wc), BF16),
        in_specs=[pl.BlockSpec(memory_space=pl.ANY)] * 6,
        out_specs=pl.BlockSpec(memory_space=pltpu.VMEM),
        scratch_shapes=[
            pltpu.SMEM((ns,), I32),
            pltpu.VMEM((ns, hl, hd), BF16),
            pltpu.VMEM((pages * rows, hd), BF16),
            pltpu.VMEM((pages * rows, hd), BF16),
            pltpu.VMEM((pr, LANES), I32),
            pltpu.VMEM((cores, wr, wc), BF16),
            pltpu.VMEM((pr, LANES), F32),
            pltpu.VMEM((8, LANES), I32),
            pltpu.SMEM((8, LANES), I32),
            pltpu.VMEM((hl, rows), I32),
            pltpu.VMEM((pages, hl, rows), BF16),
            pltpu.VMEM((pages, hl, LANES), F32),
            pltpu.VMEM((pages, hl, LANES), F32),
            pltpu.VMEM((pages + 1, hl, LANES), F32),
            pltpu.VMEM((pages + 1, hl, LANES), F32),
            pltpu.VMEM((pages + 1, hl, hd), F32),
            pltpu.VMEM((ns, hl, hd), F32),
            pltpu.VMEM((cores * nx * 2, hh + 1, sb, hd), BF16),
            pltpu.VMEM((cores * nx * 2, hh + 1, sb, hd), BF16),
            pltpu.VMEM((cores * hh + 1, sb, hd), BF16),
            pltpu.VMEM((nz // 2, cores * hh + 1, sb, hd), BF16),
            pltpu.VMEM((nx, 2, cores * hh, sb, hd), BF16),
            dma, dma, dma((len(K_PARTS),)), dma((len(V_PARTS),)), dma, dma, dma, dma, dma,
            dma, dma, dma, dma, dma, dma, dma((2,)), dma((2,)),
        ],
        compiler_params=pltpu.CompilerParams(collective_id=0, has_side_effects=True),
        name="paged_decode",
    )(
        lengths, query, key_cache.reshape(pages * rows, hd), value_cache.reshape(pages * rows, hd),
        page_order.reshape(pr, LANES), out_weight)


def solution(mesh):
    in_specs = (
        P("group", "tensor", None),
        P(("group", "seq"), None, "tensor", None),
        P(("group", "seq"), None, "tensor", None),
        P("group"),
        P("group"),
        P("tensor", "seq"),
    )
    out_specs = P(("group", "tensor"), "seq")
    return jax.shard_map(body, mesh=mesh, in_specs=in_specs, out_specs=out_specs, check_vma=False)
```

```python
import functools
import math

import jax
import jax.numpy as jnp
from jax import lax
from jax.experimental import pallas as pl
from jax.experimental.pallas import tpu as pltpu
from jax.sharding import PartitionSpec as P

MESH = pl.DeviceIdType.MESH
F32 = jnp.float32
BF16 = jnp.bfloat16
I32 = jnp.int32
LANES = 128
NEG = -1e30
K_PARTS = (12, 20)
V_PARTS = (32,)


def kernel(
    dims,
    len_hbm, q_hbm, k_hbm, v_hbm, po_hbm, w_hbm, out_ref,
    len_s, q_v, k_v, v_v, po_v, w_v, val_v, meta_v, meta_s, cmod_v,
    wt_v, mtop, ltot, mrun, lrun, orun, ofin, s1, r1, s2, r2, g_v,
    len_sem, q_sem, k_sem, v_sem, po_sem, w_sem, meta_sem, ws_sem, wr_sem,
    s1s_sem, s1r_sem, s2s_sem, s2r_sem, gzs_sem, gxs_sem, own_sem, peer_sem,
):
    nx, nz, pages, page_len, kvh, ns, hl, hd, cores = dims
    rows = page_len * kvh
    hq = hl // nx
    sb = ns // cores
    group_size = hl // kvh
    scale = math.log2(math.e) / math.sqrt(hd)
    me = lax.axis_index("seq")
    t = lax.axis_index("tensor")
    x = me // nz
    z = me % nz
    spots = (1, 0)
    zp = z % 2
    hh = hq // 2

    def at(px, pz, pt):
        return {"seq": px * nz + pz, "tensor": pt}

    def remote(src, dst, send, recv, to):
        return pltpu.make_async_remote_copy(
            src_ref=src, dst_ref=dst, send_sem=send, recv_sem=recv, device_id=to, device_id_type=MESH)

    len_copy = pltpu.make_async_copy(len_hbm, len_s, len_sem)
    len_copy.start()
    po_copy = pltpu.make_async_copy(po_hbm, po_v, po_sem)
    po_copy.start()
    q_copy = pltpu.make_async_copy(q_hbm, q_v, q_sem)
    q_copy.start()

    peers = []
    for dx in [nx // 2] + [d for d in range(nx) if d != nx // 2]:
        for dp in range(2):
            for dt in range(cores):
                if dx or dp or dt:
                    peers.append(((x + dx) % nx, (zp + dp) % 2, (t + dt) % cores))
    barrier = pltpu.get_barrier_semaphore()

    def greet(px, pz, pt):
        pl.semaphore_signal(barrier, inc=1, device_id=at(px, pz, pt), device_id_type=MESH)

    early_greets = 4
    for px, pp, pt in peers[:early_greets]:
        greet(px, z - zp + pp, pt)

    def kv_copies(src, dst, sem, shares):
        copies, first = [], 0
        for i, share in enumerate(shares):
            count = pages * share // sum(shares)
            part = pl.ds(first * rows, count * rows)
            copies.append((pltpu.make_async_copy(src.at[part], dst.at[part], sem.at[i]), range(first, first + count)))
            first += count
        return copies

    k_copies = kv_copies(k_hbm, k_v, k_sem, K_PARTS)
    v_copies = kv_copies(v_hbm, v_v, v_sem, V_PARTS)
    for copy, _ in k_copies + v_copies:
        copy.start()
    w_copy = pltpu.make_async_copy(w_hbm, w_v.at[t], w_sem)
    w_copy.start()

    for px, pp, pt in peers[early_greets:]:
        greet(px, z - zp + pp, pt)

    @pl.when(z < 2)
    def _():
        for d in range(2, nz, 2):
            greet(x, z + d, t)

    cl = lax.broadcasted_iota(I32, (hl, rows), 1)
    hr = lax.broadcasted_iota(I32, (hl, rows), 0)
    cmod_v[...] = jnp.where(cl % kvh == hr // group_size, cl, 1 << 20)
    mrun[0] = jnp.full((hl, LANES), NEG, F32)
    lrun[0] = jnp.zeros((hl, LANES), F32)
    orun[0] = jnp.zeros((hl, hd), F32)

    len_copy.wait()
    lens = [len_s[s] for s in range(ns)]
    starts = []
    run = jnp.int32(0)
    for s in range(ns):
        starts.append(run)
        run = run + lax.shift_right_logical(lens[s] + (page_len - 1), int(math.log2(page_len)))
    pr = po_v.shape[0]
    rank = lax.broadcasted_iota(I32, (pr, LANES), 0) * LANES + lax.broadcasted_iota(I32, (pr, LANES), 1)
    owner = jnp.zeros((pr, LANES), I32)
    end = jnp.full((pr, LANES), lens[0], I32)
    for s in range(1, ns):
        past = rank >= starts[s]
        owner = jnp.where(past, s, owner)
        end = jnp.where(past, lens[s] + starts[s] * page_len, end)
    valid = jnp.clip(end - rank * page_len, 0, page_len)
    owner = jnp.where(valid > 0, owner, ns)
    val_v[...] = (owner * 256 + valid).astype(F32)

    po_copy.wait()
    ids = lax.broadcasted_iota(I32, (pages, LANES), 0) + me * pages
    acc = jnp.zeros((pages, LANES), F32)
    for i in range(pr):
        hit = jnp.broadcast_to(po_v[i : i + 1, :], (pages, LANES)) == ids
        acc = acc + jnp.where(hit, jnp.broadcast_to(val_v[i : i + 1, :], (pages, LANES)), 0.0)
    val_col = jnp.broadcast_to(jnp.sum(acc, axis=1, keepdims=True), (pages, LANES))
    pad = jnp.concatenate([val_col, jnp.zeros((LANES - pages, LANES), F32)], axis=0)
    val_row = jnp.transpose(pad)[0:1, :]
    own_col = lax.shift_right_logical(val_col.astype(I32), 8)
    val_row_i = val_row.astype(I32)
    own_row = lax.shift_right_logical(val_row_i, 8)
    prow = lax.broadcasted_iota(I32, (pages, LANES), 0)
    lane = lax.broadcasted_iota(I32, (pages, LANES), 1)
    same = (own_col == jnp.broadcast_to(own_row, (pages, LANES))) & (prow < lane)
    prev = jnp.max(jnp.where(same, (prow + 1).astype(F32), 0.0), axis=0, keepdims=True).astype(I32)
    last = jnp.max(jnp.where(own_col == lane, (prow + 1).astype(F32), 0.0), axis=0, keepdims=True).astype(I32)
    meta_v[0:1, :] = prev * 8192 + val_row_i
    meta_v[1:2, :] = last
    meta_copy = pltpu.make_async_copy(meta_v, meta_s, meta_sem)
    meta_copy.start()
    meta_copy.wait()
    q_copy.wait()

    def page_part(p):
        return pl.ds(p * rows, rows)

    for copy, part in k_copies:
        copy.wait()
        for p in part:
            code = meta_s[0, p]
            nvalid = jnp.bitwise_and(code, 255) * kvh
            own = jnp.minimum(jnp.bitwise_and(lax.shift_right_logical(code, 8), 31), ns - 1)
            before = jnp.clip(lax.shift_right_logical(code, 13), 0, pages)
            sc = lax.dot_general(
                q_v[own], k_v[page_part(p), :], (((1,), (1,)), ((), ())), preferred_element_type=F32)
            sc = jnp.where(cmod_v[...] < nvalid, sc, NEG)
            top = jnp.max(sc, axis=1, keepdims=True)
            wt = jnp.exp2((sc - top) * scale)
            wt_v[p] = wt.astype(BF16)
            top = jnp.broadcast_to(top, (hl, LANES))
            mtop[p] = top
            ltot[p] = jnp.broadcast_to(jnp.sum(wt, axis=1, keepdims=True), (hl, LANES))
            mrun[p + 1] = jnp.maximum(mrun[before], top)

    for copy, part in v_copies:
        copy.wait()
        for p in part:
            code = meta_s[0, p]
            own = jnp.bitwise_and(lax.shift_right_logical(code, 8), 31)
            before = jnp.clip(lax.shift_right_logical(code, 13), 0, pages)
            final = jnp.clip(meta_s[1, own], 0, pages)
            o = jnp.dot(wt_v[p], v_v[page_part(p), :], preferred_element_type=F32)
            fb = jnp.exp2((mtop[p] - mrun[final]) * scale)
            lrun[p + 1] = lrun[before] + fb * ltot[p]
            orun[p + 1] = orun[before] + fb * o

    lane_h = lax.broadcasted_iota(I32, (hl, LANES), 1)
    half = LANES // 2
    ml = jnp.zeros((hl, LANES), F32)
    for s in range(ns):
        f = jnp.clip(meta_s[1, s], 0, pages)
        ofin[s] = orun[f]
        ml = jnp.where(lane_h == s, mrun[f], ml)
        ml = jnp.where(lane_h == half + s, lrun[f], ml)
    hn = cores * hh
    row_h = lax.broadcasted_iota(I32, (hn, LANES), 0)
    lane_r = lax.broadcasted_iota(I32, (hn, LANES), 1)

    def split(v):
        a = v.astype(BF16).astype(F32)
        b = (v - a).astype(BF16).astype(F32)
        return a + pltpu.roll(b, ns, 1) + pltpu.roll(v - a - b, 2 * ns, 1)

    def joined(v):
        return v + pltpu.roll(v, LANES - ns, 1) + pltpu.roll(v, LANES - 2 * ns, 1)

    ml = split(ml)
    for cx in range(nx):
        for cp in range(2):
            h0 = cx * hq + cp * hh
            tail = jnp.concatenate([ml[h0 : h0 + hh]] * cores, axis=0)
            tail = jnp.where(row_h // hh == t, tail, 0.0).astype(BF16)
            for ct in range(cores):
                d = (cx * 2 + cp) * cores + ct
                s1[d, hh] = tail
                for j in range(hh):
                    s1[d, j] = ofin[ct * sb : (ct + 1) * sb, h0 + j, :].astype(BF16)
    here = (t * nx + x) * 2 + zp
    r1[here] = s1[(x * 2 + zp) * cores + t]

    pl.semaphore_wait(barrier, len(peers) + jnp.where(z < 2, 0, 1))

    for px, pp, pt in peers:
        remote(s1.at[(px * 2 + pp) * cores + pt], r1.at[here], s1s_sem, s1r_sem, at(px, z - zp + pp, pt)).start()

    def bulk(ref, blocks, send, recv):
        part = ref.at[pl.ds(0, blocks)]
        return remote(part, part, send, recv, at(x, z, (t + 1) % cores))

    bulk(r1, len(peers), s1s_sem, s1r_sem).wait_recv()

    def merged(ml):
        top = functools.reduce(jnp.maximum, ml)
        fs = [jnp.exp2((m - top) * scale) for m in ml]
        tot = functools.reduce(jnp.add, [f * pltpu.roll(m, half, 1) for f, m in zip(fs, ml)])
        return top, fs, tot

    def as_columns(fs):
        pad = jnp.zeros((LANES - len(fs) * hn, LANES), F32)
        ft = jnp.transpose(jnp.concatenate(fs + [pad], axis=0))
        return jnp.where(t == 0, ft[:sb], ft[sb : 2 * sb])

    def source_ml(i):
        return joined(r1[i, hh].astype(F32) + r1[nx * 2 + i, hh].astype(F32))

    top, fs, tot = merged([source_ml(i) for i in range(nx * 2)])
    out_ml = jnp.where(lane_r < half, top, pltpu.roll(tot, half, 1))
    s2[hn] = split(jnp.where(lane_r % half < ns, out_ml, 0.0)).astype(BF16)
    ft = as_columns(fs)
    for ct in range(cores):
        for j in range(hh):
            k = ct * hh + j
            num = functools.reduce(
                jnp.add,
                [jnp.broadcast_to(ft[:, i * hn + k : i * hn + k + 1], (sb, hd)) * r1[ct * nx * 2 + i, j].astype(F32)
                 for i in range(nx * 2)])
            s2[k] = num.astype(BF16)

    @pl.when(z >= 2)
    def _():
        remote(s2, r2.at[z // 2], s2s_sem, s2r_sem, at(x, zp, t)).start()

    @pl.when(z < 2)
    def _():
        r2[0] = s2[...]

    bulk(s1, len(peers), s1s_sem, s1r_sem).wait_send()

    @pl.when(z >= 2)
    def _():
        remote(s2, s2, s2s_sem, s2r_sem, at(x, z, (t + 1) % cores)).wait_send()

    w_send = remote(w_v.at[t], w_v.at[t], ws_sem, wr_sem, at(x, z, (t + 1) % cores))
    w_recv = remote(w_v.at[t], w_v.at[(t + 1) % cores], ws_sem, wr_sem, at(x, z, (t + 1) % cores))
    w_copy.wait()
    w_send.start()

    def direct(dx):
        to = at((x + dx) % nx, spots[1], t)
        return remote(g_v.at[x, 0], g_v.at[x, 0], gzs_sem, peer_sem.at[0] if dx else own_sem.at[0], to)

    def along_z(o, pz):
        return remote(g_v.at[x, o], g_v.at[x, o], gzs_sem, own_sem.at[o], at(x, pz, t))

    def along_x(o, dx):
        return remote(g_v.at[x, o], g_v.at[x, o], gxs_sem, peer_sem.at[o], at((x + dx) % nx, z, t))

    def own_arrival(o):
        return remote(g_v.at[x, o], g_v.at[x, o], gzs_sem, own_sem.at[o], at(x, z, (t + 1) % cores))

    xorder = [d for d in range(nx) if d]
    for o in reversed(range(cores)):
        zorder = [(spots[o] + d) % nz for d in range(1, nz)]
        if o == 0:
            zorder = [pz for pz in zorder if pz != spots[1]]

        @pl.when(z == spots[o])
        def _():
            bulk(r2, nz // 2 - 1, s2s_sem, s2r_sem).wait_recv()
            top, fs, tot = merged([joined(r2[i, hn].astype(F32)) for i in range(nz // 2)])
            inv = jnp.where(lane_r < ns, 1.0 / tot, 0.0)
            ft = as_columns([f * inv for f in fs])
            for k in range(hn):
                att = functools.reduce(
                    jnp.add,
                    [jnp.broadcast_to(ft[:, i * hn + k : i * hn + k + 1], (sb, hd)) * r2[i, k].astype(F32)
                     for i in range(nz // 2)])
                g_v[x, o, k] = att.astype(BF16)
            if o == 0:
                along_z(o, zorder[0]).start()
                for dx in xorder + [0]:
                    direct(dx).start()
            else:
                for dx in xorder:
                    along_x(o, dx).start()
            for pz in zorder[1 if o == 0 else 0 :]:
                along_z(o, pz).start()
            if o == 0:
                for dx in xorder:
                    along_x(o, dx).start()

    for o in reversed(range(cores)):
        @pl.when((z != spots[o]) & ((z != spots[1]) | (o == 1)))
        def _():
            own_arrival(o).wait_recv()
            for dx in xorder:
                along_x(o, dx).start()

    w_send.wait_send()
    w_recv.wait_recv()

    def bytes_of(blocks, send, recv):
        part = k_v.at[pl.ds(0, blocks * hn * sb)]
        return remote(part, part, send, recv, at(x, z, (t + 1) % cores))

    out = jnp.zeros((sb, hd), F32)
    for o in reversed(range(2)):
        if o == 0:
            @pl.when(z == spots[1])
            def _():
                own_arrival(0).wait_recv()

        for dx in [0] + xorder:
            if dx == xorder[0]:
                bytes_of(nx - 1, gxs_sem, peer_sem.at[o]).wait_recv()
            sx = (x + dx) % nx
            for k in range(0, hn, 2):
                lhs = jnp.concatenate([g_v[sx, o, k], g_v[sx, o, k + 1]], axis=1)
                head = sx * hq + (1 - o) * hh + k % hh
                first = pl.multiple_of(head * hd, 2 * hd)
                out = out + jnp.dot(lhs, w_v[k // hh, pl.ds(first, 2 * hd), :], preferred_element_type=F32)
    out_ref[...] = out.astype(out_ref.dtype)

    @pl.when(z == spots[0])
    def _():
        bytes_of(nz - 2 + nx, gzs_sem, own_sem.at[0]).wait_send()

    @pl.when(z == spots[1])
    def _():
        bytes_of(nz - 1, gzs_sem, own_sem.at[0]).wait_send()
        bytes_of(nx - 1, gxs_sem, peer_sem.at[1]).wait_send()

    @pl.when(z != spots[1])
    def _():
        bytes_of(cores * (nx - 1), gxs_sem, peer_sem.at[0]).wait_send()


def body(query, key_cache, value_cache, lengths, page_order, out_weight):
    pages, page_len, kvh, hd = key_cache.shape
    ns, hl = query.shape[0], query.shape[1]
    cores = lax.axis_size("tensor")
    nz = ns
    nx = lax.axis_size("seq") // nz
    hh = hl // nx // 2
    sb = ns // cores
    rows = page_len * kvh
    pr = page_order.shape[0] // LANES
    wr, wc = out_weight.shape
    dims = (nx, nz, pages, page_len, kvh, ns, hl, hd, cores)
    dma = pltpu.SemaphoreType.DMA
    return pl.pallas_call(
        functools.partial(kernel, dims),
        out_shape=pltpu.VMEM((sb, wc), BF16),
        in_specs=[pl.BlockSpec(memory_space=pl.ANY)] * 6,
        out_specs=pl.BlockSpec(memory_space=pltpu.VMEM),
        scratch_shapes=[
            pltpu.SMEM((ns,), I32),
            pltpu.VMEM((ns, hl, hd), BF16),
            pltpu.VMEM((pages * rows, hd), BF16),
            pltpu.VMEM((pages * rows, hd), BF16),
            pltpu.VMEM((pr, LANES), I32),
            pltpu.VMEM((cores, wr, wc), BF16),
            pltpu.VMEM((pr, LANES), F32),
            pltpu.VMEM((8, LANES), I32),
            pltpu.SMEM((8, LANES), I32),
            pltpu.VMEM((hl, rows), I32),
            pltpu.VMEM((pages, hl, rows), BF16),
            pltpu.VMEM((pages, hl, LANES), F32),
            pltpu.VMEM((pages, hl, LANES), F32),
            pltpu.VMEM((pages + 1, hl, LANES), F32),
            pltpu.VMEM((pages + 1, hl, LANES), F32),
            pltpu.VMEM((pages + 1, hl, hd), F32),
            pltpu.VMEM((ns, hl, hd), F32),
            pltpu.VMEM((cores * nx * 2, hh + 1, sb, hd), BF16),
            pltpu.VMEM((cores * nx * 2, hh + 1, sb, hd), BF16),
            pltpu.VMEM((cores * hh + 1, sb, hd), BF16),
            pltpu.VMEM((nz // 2, cores * hh + 1, sb, hd), BF16),
            pltpu.VMEM((nx, 2, cores * hh, sb, hd), BF16),
            dma, dma, dma((len(K_PARTS),)), dma((len(V_PARTS),)), dma, dma, dma, dma, dma,
            dma, dma, dma, dma, dma, dma, dma((2,)), dma((2,)),
        ],
        compiler_params=pltpu.CompilerParams(collective_id=0, has_side_effects=True),
        name="paged_decode",
    )(
        lengths, query, key_cache.reshape(pages * rows, hd), value_cache.reshape(pages * rows, hd),
        page_order.reshape(pr, LANES), out_weight)


def solution(mesh):
    in_specs = (
        P("group", "tensor", None),
        P(("group", "seq"), None, "tensor", None),
        P(("group", "seq"), None, "tensor", None),
        P("group"),
        P("group"),
        P("tensor", "seq"),
    )
    out_specs = P(("group", "tensor"), "seq")
    return jax.shard_map(body, mesh=mesh, in_specs=in_specs, out_specs=out_specs, check_vma=False)
```

```python
import functools
import math

import jax
import jax.numpy as jnp
from jax import lax
from jax.experimental import pallas as pl
from jax.experimental.pallas import tpu as pltpu
from jax.sharding import PartitionSpec as P

MESH = pl.DeviceIdType.MESH
F32 = jnp.float32
BF16 = jnp.bfloat16
I32 = jnp.int32
LANES = 128
NEG = -1e30
K_PARTS = (10, 22)
V_PARTS = (32,)


def kernel(
    dims,
    len_hbm, q_hbm, k_hbm, v_hbm, po_hbm, w_hbm, out_ref,
    len_s, q_v, k_v, v_v, po_v, w_v, val_v, meta_v, meta_s, cmod_v,
    wt_v, mtop, ltot, mrun, lrun, orun, ofin, s1, r1, s2, r2, g_v,
    len_sem, q_sem, k_sem, v_sem, po_sem, w_sem, meta_sem, ws_sem, wr_sem,
    s1s_sem, s1r_sem, s2s_sem, s2r_sem, gzs_sem, gxs_sem, own_sem, peer_sem,
):
    nx, nz, pages, page_len, kvh, ns, hl, hd, cores = dims
    rows = page_len * kvh
    hq = hl // nx
    sb = ns // cores
    group_size = hl // kvh
    scale = math.log2(math.e) / math.sqrt(hd)
    me = lax.axis_index("seq")
    t = lax.axis_index("tensor")
    x = me // nz
    z = me % nz
    spots = (1, 0)
    zp = z % 2
    hh = hq // 2

    def at(px, pz, pt):
        return {"seq": px * nz + pz, "tensor": pt}

    def remote(src, dst, send, recv, to):
        return pltpu.make_async_remote_copy(
            src_ref=src, dst_ref=dst, send_sem=send, recv_sem=recv, device_id=to, device_id_type=MESH)

    len_copy = pltpu.make_async_copy(len_hbm, len_s, len_sem)
    len_copy.start()
    po_copy = pltpu.make_async_copy(po_hbm, po_v, po_sem)
    po_copy.start()
    q_copy = pltpu.make_async_copy(q_hbm, q_v, q_sem)
    q_copy.start()

    peers = []
    for dx in [nx // 2] + [d for d in range(nx) if d != nx // 2]:
        for dp in range(2):
            for dt in range(cores):
                if dx or dp or dt:
                    peers.append(((x + dx) % nx, (zp + dp) % 2, (t + dt) % cores))
    barrier = pltpu.get_barrier_semaphore()

    def greet(px, pz, pt):
        pl.semaphore_signal(barrier, inc=1, device_id=at(px, pz, pt), device_id_type=MESH)

    early_greets = 4
    for px, pp, pt in peers[:early_greets]:
        greet(px, z - zp + pp, pt)

    def kv_copies(src, dst, sem, shares):
        copies, first = [], 0
        for i, share in enumerate(shares):
            count = pages * share // sum(shares)
            part = pl.ds(first * rows, count * rows)
            copies.append((pltpu.make_async_copy(src.at[part], dst.at[part], sem.at[i]), range(first, first + count)))
            first += count
        return copies

    k_copies = kv_copies(k_hbm, k_v, k_sem, K_PARTS)
    v_copies = kv_copies(v_hbm, v_v, v_sem, V_PARTS)
    for copy, _ in k_copies + v_copies:
        copy.start()
    w_copy = pltpu.make_async_copy(w_hbm, w_v.at[t], w_sem)
    w_copy.start()

    for px, pp, pt in peers[early_greets:]:
        greet(px, z - zp + pp, pt)

    @pl.when(z < 2)
    def _():
        for d in range(2, nz, 2):
            greet(x, z + d, t)

    cl = lax.broadcasted_iota(I32, (hl, rows), 1)
    hr = lax.broadcasted_iota(I32, (hl, rows), 0)
    cmod_v[...] = jnp.where(cl % kvh == hr // group_size, cl, 1 << 20)
    mrun[0] = jnp.full((hl, LANES), NEG, F32)
    lrun[0] = jnp.zeros((hl, LANES), F32)
    orun[0] = jnp.zeros((hl, hd), F32)

    len_copy.wait()
    lens = [len_s[s] for s in range(ns)]
    starts = []
    run = jnp.int32(0)
    for s in range(ns):
        starts.append(run)
        run = run + lax.shift_right_logical(lens[s] + (page_len - 1), int(math.log2(page_len)))
    pr = po_v.shape[0]
    rank = lax.broadcasted_iota(I32, (pr, LANES), 0) * LANES + lax.broadcasted_iota(I32, (pr, LANES), 1)
    owner = jnp.zeros((pr, LANES), I32)
    end = jnp.full((pr, LANES), lens[0], I32)
    for s in range(1, ns):
        past = rank >= starts[s]
        owner = jnp.where(past, s, owner)
        end = jnp.where(past, lens[s] + starts[s] * page_len, end)
    valid = jnp.clip(end - rank * page_len, 0, page_len)
    owner = jnp.where(valid > 0, owner, ns)
    val_v[...] = (owner * 256 + valid).astype(F32)

    po_copy.wait()
    ids = lax.broadcasted_iota(I32, (pages, LANES), 0) + me * pages
    acc = jnp.zeros((pages, LANES), F32)
    for i in range(pr):
        hit = jnp.broadcast_to(po_v[i : i + 1, :], (pages, LANES)) == ids
        acc = acc + jnp.where(hit, jnp.broadcast_to(val_v[i : i + 1, :], (pages, LANES)), 0.0)
    val_col = jnp.broadcast_to(jnp.sum(acc, axis=1, keepdims=True), (pages, LANES))
    pad = jnp.concatenate([val_col, jnp.zeros((LANES - pages, LANES), F32)], axis=0)
    val_row = jnp.transpose(pad)[0:1, :]
    own_col = lax.shift_right_logical(val_col.astype(I32), 8)
    val_row_i = val_row.astype(I32)
    own_row = lax.shift_right_logical(val_row_i, 8)
    prow = lax.broadcasted_iota(I32, (pages, LANES), 0)
    lane = lax.broadcasted_iota(I32, (pages, LANES), 1)
    same = (own_col == jnp.broadcast_to(own_row, (pages, LANES))) & (prow < lane)
    prev = jnp.max(jnp.where(same, (prow + 1).astype(F32), 0.0), axis=0, keepdims=True).astype(I32)
    last = jnp.max(jnp.where(own_col == lane, (prow + 1).astype(F32), 0.0), axis=0, keepdims=True).astype(I32)
    meta_v[0:1, :] = prev * 8192 + val_row_i
    meta_v[1:2, :] = last
    meta_copy = pltpu.make_async_copy(meta_v, meta_s, meta_sem)
    meta_copy.start()
    meta_copy.wait()
    q_copy.wait()

    def page_part(p):
        return pl.ds(p * rows, rows)

    for copy, part in k_copies:
        copy.wait()
        for p in part:
            code = meta_s[0, p]
            nvalid = jnp.bitwise_and(code, 255) * kvh
            own = jnp.minimum(jnp.bitwise_and(lax.shift_right_logical(code, 8), 31), ns - 1)
            before = jnp.clip(lax.shift_right_logical(code, 13), 0, pages)
            sc = lax.dot_general(
                q_v[own], k_v[page_part(p), :], (((1,), (1,)), ((), ())), preferred_element_type=F32)
            sc = jnp.where(cmod_v[...] < nvalid, sc, NEG)
            top = jnp.max(sc, axis=1, keepdims=True)
            wt = jnp.exp2((sc - top) * scale)
            wt_v[p] = wt.astype(BF16)
            top = jnp.broadcast_to(top, (hl, LANES))
            mtop[p] = top
            ltot[p] = jnp.broadcast_to(jnp.sum(wt, axis=1, keepdims=True), (hl, LANES))
            mrun[p + 1] = jnp.maximum(mrun[before], top)

    for copy, part in v_copies:
        copy.wait()
        for p in part:
            code = meta_s[0, p]
            own = jnp.bitwise_and(lax.shift_right_logical(code, 8), 31)
            before = jnp.clip(lax.shift_right_logical(code, 13), 0, pages)
            final = jnp.clip(meta_s[1, own], 0, pages)
            o = jnp.dot(wt_v[p], v_v[page_part(p), :], preferred_element_type=F32)
            fb = jnp.exp2((mtop[p] - mrun[final]) * scale)
            lrun[p + 1] = lrun[before] + fb * ltot[p]
            orun[p + 1] = orun[before] + fb * o

    lane_h = lax.broadcasted_iota(I32, (hl, LANES), 1)
    half = LANES // 2
    ml = jnp.zeros((hl, LANES), F32)
    for s in range(ns):
        f = jnp.clip(meta_s[1, s], 0, pages)
        ofin[s] = orun[f]
        ml = jnp.where(lane_h == s, mrun[f], ml)
        ml = jnp.where(lane_h == half + s, lrun[f], ml)
    hn = cores * hh
    row_h = lax.broadcasted_iota(I32, (hn, LANES), 0)
    lane_r = lax.broadcasted_iota(I32, (hn, LANES), 1)

    def split(v):
        a = v.astype(BF16).astype(F32)
        b = (v - a).astype(BF16).astype(F32)
        return a + pltpu.roll(b, ns, 1) + pltpu.roll(v - a - b, 2 * ns, 1)

    def joined(v):
        return v + pltpu.roll(v, LANES - ns, 1) + pltpu.roll(v, LANES - 2 * ns, 1)

    ml = split(ml)
    for cx in range(nx):
        for cp in range(2):
            h0 = cx * hq + cp * hh
            tail = jnp.concatenate([ml[h0 : h0 + hh]] * cores, axis=0)
            tail = jnp.where(row_h // hh == t, tail, 0.0).astype(BF16)
            for ct in range(cores):
                d = (cx * 2 + cp) * cores + ct
                s1[d, hh] = tail
                for j in range(hh):
                    s1[d, j] = ofin[ct * sb : (ct + 1) * sb, h0 + j, :].astype(BF16)
    here = (t * nx + x) * 2 + zp
    r1[here] = s1[(x * 2 + zp) * cores + t]

    pl.semaphore_wait(barrier, len(peers) + jnp.where(z < 2, 0, 1))

    for px, pp, pt in peers:
        remote(s1.at[(px * 2 + pp) * cores + pt], r1.at[here], s1s_sem, s1r_sem, at(px, z - zp + pp, pt)).start()

    def bulk(ref, blocks, send, recv):
        part = ref.at[pl.ds(0, blocks)]
        return remote(part, part, send, recv, at(x, z, (t + 1) % cores))

    bulk(r1, len(peers), s1s_sem, s1r_sem).wait_recv()

    def merged(ml):
        top = functools.reduce(jnp.maximum, ml)
        fs = [jnp.exp2((m - top) * scale) for m in ml]
        tot = functools.reduce(jnp.add, [f * pltpu.roll(m, half, 1) for f, m in zip(fs, ml)])
        return top, fs, tot

    def as_columns(fs):
        pad = jnp.zeros((LANES - len(fs) * hn, LANES), F32)
        ft = jnp.transpose(jnp.concatenate(fs + [pad], axis=0))
        return jnp.where(t == 0, ft[:sb], ft[sb : 2 * sb])

    def source_ml(i):
        return joined(r1[i, hh].astype(F32) + r1[nx * 2 + i, hh].astype(F32))

    top, fs, tot = merged([source_ml(i) for i in range(nx * 2)])
    out_ml = jnp.where(lane_r < half, top, pltpu.roll(tot, half, 1))
    s2[hn] = split(jnp.where(lane_r % half < ns, out_ml, 0.0)).astype(BF16)
    ft = as_columns(fs)
    for ct in range(cores):
        for j in range(hh):
            k = ct * hh + j
            num = functools.reduce(
                jnp.add,
                [jnp.broadcast_to(ft[:, i * hn + k : i * hn + k + 1], (sb, hd)) * r1[ct * nx * 2 + i, j].astype(F32)
                 for i in range(nx * 2)])
            s2[k] = num.astype(BF16)

    @pl.when(z >= 2)
    def _():
        remote(s2, r2.at[z // 2], s2s_sem, s2r_sem, at(x, zp, t)).start()

    @pl.when(z < 2)
    def _():
        r2[0] = s2[...]

    bulk(s1, len(peers), s1s_sem, s1r_sem).wait_send()

    @pl.when(z >= 2)
    def _():
        remote(s2, s2, s2s_sem, s2r_sem, at(x, z, (t + 1) % cores)).wait_send()

    w_send = remote(w_v.at[t], w_v.at[t], ws_sem, wr_sem, at(x, z, (t + 1) % cores))
    w_recv = remote(w_v.at[t], w_v.at[(t + 1) % cores], ws_sem, wr_sem, at(x, z, (t + 1) % cores))
    w_copy.wait()
    w_send.start()

    def direct(dx):
        to = at((x + dx) % nx, spots[1], t)
        return remote(g_v.at[x, 0], g_v.at[x, 0], gzs_sem, peer_sem.at[0] if dx else own_sem.at[0], to)

    def along_z(o, pz):
        return remote(g_v.at[x, o], g_v.at[x, o], gzs_sem, own_sem.at[o], at(x, pz, t))

    def along_x(o, dx):
        return remote(g_v.at[x, o], g_v.at[x, o], gxs_sem, peer_sem.at[o], at((x + dx) % nx, z, t))

    def own_arrival(o):
        return remote(g_v.at[x, o], g_v.at[x, o], gzs_sem, own_sem.at[o], at(x, z, (t + 1) % cores))

    xorder = [d for d in range(nx) if d]
    for o in reversed(range(cores)):
        zorder = [(spots[o] + d) % nz for d in range(1, nz)]
        if o == 0:
            zorder = [pz for pz in zorder if pz != spots[1]]

        @pl.when(z == spots[o])
        def _():
            bulk(r2, nz // 2 - 1, s2s_sem, s2r_sem).wait_recv()
            top, fs, tot = merged([joined(r2[i, hn].astype(F32)) for i in range(nz // 2)])
            inv = jnp.where(lane_r < ns, 1.0 / tot, 0.0)
            ft = as_columns([f * inv for f in fs])
            for k in range(hn):
                att = functools.reduce(
                    jnp.add,
                    [jnp.broadcast_to(ft[:, i * hn + k : i * hn + k + 1], (sb, hd)) * r2[i, k].astype(F32)
                     for i in range(nz // 2)])
                g_v[x, o, k] = att.astype(BF16)
            along_z(o, zorder[0]).start()
            if o == 0:
                for dx in xorder + [0]:
                    direct(dx).start()
            else:
                for dx in xorder:
                    along_x(o, dx).start()
            for pz in zorder[1:]:
                along_z(o, pz).start()
            if o == 0:
                for dx in xorder:
                    along_x(o, dx).start()

    for o in reversed(range(cores)):
        @pl.when((z != spots[o]) & ((z != spots[1]) | (o == 1)))
        def _():
            own_arrival(o).wait_recv()
            for dx in xorder:
                along_x(o, dx).start()

    w_send.wait_send()
    w_recv.wait_recv()

    def bytes_of(blocks, send, recv):
        part = k_v.at[pl.ds(0, blocks * hn * sb)]
        return remote(part, part, send, recv, at(x, z, (t + 1) % cores))

    out = jnp.zeros((sb, hd), F32)
    for o in reversed(range(2)):
        if o == 0:
            @pl.when(z == spots[1])
            def _():
                own_arrival(0).wait_recv()

        for dx in [0] + xorder:
            if dx == xorder[0]:
                bytes_of(nx - 1, gxs_sem, peer_sem.at[o]).wait_recv()
            sx = (x + dx) % nx
            for k in range(0, hn, 2):
                lhs = jnp.concatenate([g_v[sx, o, k], g_v[sx, o, k + 1]], axis=1)
                head = sx * hq + (1 - o) * hh + k % hh
                first = pl.multiple_of(head * hd, 2 * hd)
                out = out + jnp.dot(lhs, w_v[k // hh, pl.ds(first, 2 * hd), :], preferred_element_type=F32)
    out_ref[...] = out.astype(out_ref.dtype)

    @pl.when(z == spots[0])
    def _():
        bytes_of(nz - 2 + nx, gzs_sem, own_sem.at[0]).wait_send()

    @pl.when(z == spots[1])
    def _():
        bytes_of(nz - 1, gzs_sem, own_sem.at[0]).wait_send()
        bytes_of(nx - 1, gxs_sem, peer_sem.at[1]).wait_send()

    @pl.when(z != spots[1])
    def _():
        bytes_of(cores * (nx - 1), gxs_sem, peer_sem.at[0]).wait_send()


def body(query, key_cache, value_cache, lengths, page_order, out_weight):
    pages, page_len, kvh, hd = key_cache.shape
    ns, hl = query.shape[0], query.shape[1]
    cores = lax.axis_size("tensor")
    nz = ns
    nx = lax.axis_size("seq") // nz
    hh = hl // nx // 2
    sb = ns // cores
    rows = page_len * kvh
    pr = page_order.shape[0] // LANES
    wr, wc = out_weight.shape
    dims = (nx, nz, pages, page_len, kvh, ns, hl, hd, cores)
    dma = pltpu.SemaphoreType.DMA
    return pl.pallas_call(
        functools.partial(kernel, dims),
        out_shape=pltpu.VMEM((sb, wc), BF16),
        in_specs=[pl.BlockSpec(memory_space=pl.ANY)] * 6,
        out_specs=pl.BlockSpec(memory_space=pltpu.VMEM),
        scratch_shapes=[
            pltpu.SMEM((ns,), I32),
            pltpu.VMEM((ns, hl, hd), BF16),
            pltpu.VMEM((pages * rows, hd), BF16),
            pltpu.VMEM((pages * rows, hd), BF16),
            pltpu.VMEM((pr, LANES), I32),
            pltpu.VMEM((cores, wr, wc), BF16),
            pltpu.VMEM((pr, LANES), F32),
            pltpu.VMEM((8, LANES), I32),
            pltpu.SMEM((8, LANES), I32),
            pltpu.VMEM((hl, rows), I32),
            pltpu.VMEM((pages, hl, rows), BF16),
            pltpu.VMEM((pages, hl, LANES), F32),
            pltpu.VMEM((pages, hl, LANES), F32),
            pltpu.VMEM((pages + 1, hl, LANES), F32),
            pltpu.VMEM((pages + 1, hl, LANES), F32),
            pltpu.VMEM((pages + 1, hl, hd), F32),
            pltpu.VMEM((ns, hl, hd), F32),
            pltpu.VMEM((cores * nx * 2, hh + 1, sb, hd), BF16),
            pltpu.VMEM((cores * nx * 2, hh + 1, sb, hd), BF16),
            pltpu.VMEM((cores * hh + 1, sb, hd), BF16),
            pltpu.VMEM((nz // 2, cores * hh + 1, sb, hd), BF16),
            pltpu.VMEM((nx, 2, cores * hh, sb, hd), BF16),
            dma, dma, dma((len(K_PARTS),)), dma((len(V_PARTS),)), dma, dma, dma, dma, dma,
            dma, dma, dma, dma, dma, dma, dma((2,)), dma((2,)),
        ],
        compiler_params=pltpu.CompilerParams(collective_id=0, has_side_effects=True),
        name="paged_decode",
    )(
        lengths, query, key_cache.reshape(pages * rows, hd), value_cache.reshape(pages * rows, hd),
        page_order.reshape(pr, LANES), out_weight)


def solution(mesh):
    in_specs = (
        P("group", "tensor", None),
        P(("group", "seq"), None, "tensor", None),
        P(("group", "seq"), None, "tensor", None),
        P("group"),
        P("group"),
        P("tensor", "seq"),
    )
    out_specs = P(("group", "tensor"), "seq")
    return jax.shard_map(body, mesh=mesh, in_specs=in_specs, out_specs=out_specs, check_vma=False)
```
